256 devices in a mesh: section: 8 (over z), tm: 32 (over y, x, core).
Axes of the slice: x: 4, y: 4, z: 8, core: 2. Of those that a mesh axis runs over, the one named last changes fastest.
Arguments:
- clean: float32 [4, 4, 2048], P(None, None, 'tm'), may hold values from -6 to 6
- noise: float32 [4, 4, 2048], P(None, None, 'tm'), may hold values from -6 to 6
- timestep: int32 [4], replicated, may hold values from 0 to 999
- lift: float32 [256], replicated, may hold values from -4 to 4
- norm_gain: float32 [8, 2, 256], P('section'), may hold values from 0.5 to 1.5
- norm_bias: float32 [8, 2, 256], P('section'), may hold values from -0.7 to 0.7
- conv_weight: bfloat16 [8, 2, 3, 3, 256, 256], P('section'), may hold values from -0.125 to 0.125
- time_proj: bfloat16 [8, 256, 256], P('section'), may hold values from -0.375 to 0.375
Outputs:
- skips: bfloat16 [8, 4, 4, 2048, 256], P('section', None, None, 'tm')
The draws below stay inside these ranges and needn't reach their ends.
All inputs are finite; a program needn't handle non-finite values.
Results may differ from the reference program's by a relative error of at most 0.012.
Values may be sent and summed in bfloat16 or wider, within the bound.
No kernel may reach another device: no remote copies, remote signals or barrier semaphores. Data moves between devices by JAX's collectives and lax.ppermute only.
A program may use at most 64 MiB of HBM per device.

```python
import math
import jax
import jax.numpy as jnp
from jax import lax

C = 256
GROUPS = 32
LAYERS = 2
MB = 4
FR = 4
STEPS = 1000
TD = 64
TIME = 2048
N_SECTION = 8


def envelope(key):
    blocks = TIME // TD
    level_key, start_key = jax.random.split(jax.random.fold_in(key, 7001))
    log_level = jax.random.uniform(level_key, (MB, blocks), jnp.float32, -3.0, 1.5)
    run_length = min(3, blocks)
    run_start = jax.random.randint(start_key, (MB, 1), 0, blocks)
    positions = jnp.arange(blocks, dtype=jnp.int32)[None, :]
    silent = (positions - run_start) % blocks < run_length
    log_level = jnp.where(silent, -3.0, log_level)
    amplitude = jnp.exp(log_level)
    return jnp.repeat(amplitude, TD, axis=1)[:, None, :]


def draw_clean(key, part):
    amplitude = envelope(key)
    entry_key = jax.random.fold_in(key, 7002)
    entries = jax.random.normal(entry_key, (MB, FR, TIME), jnp.float32)
    return jnp.clip(entries * amplitude, -6.0, 6.0)


def draw_noise(key, part):
    amplitude = envelope(key)
    entry_key = jax.random.fold_in(key, 7003)
    entries = jax.random.normal(entry_key, (MB, FR, TIME), jnp.float32)
    return jnp.clip(entries * amplitude, -6.0, 6.0)


def touch_ends(drawn, stream_key, least, largest):
    spot = [jax.random.randint(jax.random.fold_in(stream_key, axis), (), 0, length) for axis, length in enumerate(drawn.shape)]
    main_axis = drawn.shape.index(max(drawn.shape))
    next_to = spot[:main_axis] + [(spot[main_axis] + 1) % drawn.shape[main_axis]] + spot[main_axis + 1:]
    return drawn.at[tuple(spot)].set(least).at[tuple(next_to)].set(largest)


def steps_of(rng, shape, shards, low, largest):
    factor_of = 1.0
    for dim, shards_of in shards:
        heights = jax.random.uniform(jax.random.fold_in(jax.random.fold_in(rng, 6), dim), (shards_of,), jnp.float32, low / len(shards), largest / len(shards))
        factor_of = factor_of * jnp.repeat(jnp.exp(heights), shape[dim] // shards_of).reshape((-1,) + (1,) * (len(shape) - 1 - dim))
    return factor_of


def normal_values(rng, extent, scale, bound, cuts=(), held_as=jnp.bfloat16):
    level = steps_of(rng, extent, cuts, -0.22, 0.18) if cuts else 1.0
    result = jax.random.normal(rng, extent, jnp.float32) * scale * level
    return jnp.minimum(jnp.maximum(result, -bound), bound).astype(held_as)


def setup_inputs(seed: int = 0) -> dict:
    splits = jax.random.split(jax.random.key(seed), 9)
    return {
        "clean": draw_clean(jax.random.fold_in(splits[8], 71), 0),
        "noise": draw_noise(jax.random.fold_in(splits[8], 71), 0),
        "timestep": touch_ends(jax.random.randint(splits[2], (MB,), 0, STEPS), jax.random.fold_in(splits[2], 1), 0, STEPS - 1).astype(jnp.int32),
        "lift": normal_values(splits[3], (C,), 1.0, 4.0, (), jnp.float32),
        "norm_gain": jnp.clip(1.0 + 0.1 * jax.random.normal(splits[4], (N_SECTION, LAYERS, C), jnp.float32), 0.5, 1.5),
        "norm_bias": jnp.clip(jax.random.uniform(splits[5], (N_SECTION, LAYERS, C), jnp.float32, -0.7, 0.7) * steps_of(splits[5], (N_SECTION, LAYERS, C), ((0, 8),), -0.4, 0.0), -0.7, 0.7),
        "conv_weight": normal_values(splits[6], (N_SECTION, LAYERS, 3, 3, C, C), (9 * C) ** -0.5, 0.125, ((0, 8),)),
        "time_proj": normal_values(splits[7], (N_SECTION, C, C), C ** -0.5, 0.375, ((0, 8),)),
    }


def prepare(clean, noise, timestep, lift):
    steps_f = timestep.astype(jnp.float32)
    level = jnp.cos(math.pi / 2.0 * (steps_f / STEPS + 0.008) / 1.008) ** 2
    noisy = jnp.sqrt(level)[:, None, None] * clean + jnp.sqrt(1.0 - level)[:, None, None] * noise
    lifted = (noisy[..., None] * lift).astype(jnp.bfloat16)
    half = C // 2
    freqs = jnp.exp(-math.log(10000.0) * jnp.arange(half, dtype=jnp.float32) / half)
    angles = steps_f[:, None] * freqs[None, :]
    emb = jnp.concatenate([jnp.sin(angles), jnp.cos(angles)], axis=1).astype(jnp.bfloat16)
    return (lifted, emb)

def group_act(h, gain, bias):
    rows_f, rows_t, width = h.shape
    grouped = h.reshape(rows_f, rows_t, GROUPS, width // GROUPS)
    count = rows_f * rows_t * (width // GROUPS)
    total = lax.optimization_barrier(jnp.sum(grouped, axis=(0, 1, 3)))
    square = lax.optimization_barrier(jnp.sum(grouped * grouped, axis=(0, 1, 3)))
    mean = total / count
    var = square / count - mean * mean
    inv = lax.rsqrt(var + 1e-05)
    normed = ((grouped - mean[:, None]) * inv[:, None]).reshape(h.shape) * gain + bias
    return jax.nn.silu(normed).astype(jnp.bfloat16)

def conv_same(padded, weight):
    rows_f = padded.shape[0]
    width_out = padded.shape[1] - 2
    chans = padded.shape[2]
    framed = jnp.pad(padded, ((1, 1), (0, 0), (0, 0)))
    total = jnp.zeros((rows_f * width_out, weight.shape[3]), jnp.float32)
    for i in range(3):
        for j in range(3):
            window = framed[i:i + rows_f, j:j + width_out].reshape(-1, chans)
            total = total + jnp.dot(window, weight[i, j], preferred_element_type=jnp.float32)
    return total.reshape(rows_f, width_out, weight.shape[3])

def reference(clean, noise, timestep, lift, norm_gain, norm_bias, conv_weight, time_proj):
    lifted, emb = prepare(clean, noise, timestep, lift)
    levels = []
    for section_id in range(N_SECTION):
        levels.append(jnp.dot(emb, time_proj[section_id], preferred_element_type=jnp.float32))
    results = []
    for micro in range(MB):
        current = lifted[micro]
        per_level = []
        for section_id in range(N_SECTION):
            depth = LAYERS if section_id < N_SECTION // 2 else 1
            hidden = current.astype(jnp.float32) + levels[section_id][micro]
            for layer in range(depth):
                act = group_act(hidden, norm_gain[section_id, layer], norm_bias[section_id, layer])
                padded = jnp.pad(act, ((0, 0), (1, 1), (0, 0)))
                hidden = hidden + conv_same(padded, conv_weight[section_id, layer])
            current = hidden.astype(jnp.bfloat16)
            per_level.append(current)
        results.append(jnp.stack(per_level))
    return jnp.stack(results, axis=1)
```

```python
import functools
import math

import jax
import jax.numpy as jnp
from jax import lax
from jax.experimental import pallas as pl
from jax.experimental.pallas import tpu as pltpu
from jax.sharding import Mesh
from jax.sharding import PartitionSpec as P

C = 256
STEPS = 1000
NZ, NY, NX, NC = 8, 4, 4, 2
FR = 4
OWN = 256
HALO = 16
STRIPS = 16
SPAN = (OWN + 2 * HALO) // STRIPS
ROWS = STRIPS * SPAN
POSITIONS = FR * OWN * NX * NC
COUNT = POSITIONS * 8
TM = ("y", "x", "c")


def group_total(x):
    lane = lax.broadcasted_iota(jnp.int32, x.shape, 1)
    for step in (1, 2, 4):
        up = pltpu.roll(x, C - step, 1)
        down = pltpu.roll(x, step, 1)
        x = x + jnp.where((lane & step) == 0, up, down)
    return x


def layer_kernel(first, last, h_ref, s0, s1, s2, s3, par_ref, valid_ref, own_ref, w_hbm, out_ref, sums_ref, act, w_ref, sem):
    fetch = pltpu.make_async_copy(w_hbm, w_ref, sem)
    fetch.start()
    sums = (s0[...] + s1[...]) + (s2[...] + s3[...])
    total, square = sums[0:1], sums[1:2]
    gain, bias, temb = par_ref[0:1], par_ref[1:2], par_ref[2:3]
    if first:
        square = square + 2.0 * temb * total + POSITIONS * temb * temb
        total = total + POSITIONS * temb
    both = group_total(jnp.concatenate([total, square, sums[2:8]], axis=0))
    mean = both[0:1] / COUNT
    var = both[1:2] / COUNT - mean * mean
    scale = lax.rsqrt(var + 1e-05) * gain
    for f in range(FR):
        for lo in range(0, ROWS, 2 * STRIPS):
            hi = lo + 2 * STRIPS
            h = h_ref[f, lo:hi].astype(jnp.float32)
            if first:
                h = h + temb
            x = (h - mean) * scale + bias
            half = 0.5 * x
            a = (half + half * jnp.tanh(half)) * valid_ref[lo:hi]
            b = a.astype(jnp.bfloat16)
            act[f, lo:hi, C : 2 * C] = b
            if hi < ROWS:
                act[f, lo + STRIPS : hi + STRIPS, 0:C] = b
            else:
                act[f, hi - STRIPS : hi, 0:C] = b[:STRIPS]
                act[f, 0:STRIPS, 0:C] = pltpu.roll(a[STRIPS:], 1, 0).astype(jnp.bfloat16)
            if lo > 0:
                act[f, lo - STRIPS : hi - STRIPS, 2 * C : 3 * C] = b
            else:
                act[f, 0:STRIPS, 2 * C : 3 * C] = b[STRIPS:]
                act[f, ROWS - STRIPS : ROWS, 2 * C : 3 * C] = pltpu.roll(a[:STRIPS], STRIPS - 1, 0).astype(jnp.bfloat16)
    fetch.wait()
    total = jnp.zeros((8, C), jnp.float32)
    square = jnp.zeros((8, C), jnp.float32)
    for f in range(FR):
        h = h_ref[f].astype(jnp.float32)
        if first:
            h = h + temb
        for i in range(3):
            if 0 <= f + i - 1 < FR:
                h = h + jnp.dot(act[f + i - 1], w_ref[i], preferred_element_type=jnp.float32)
        if last:
            low = h.astype(jnp.bfloat16)
            out_ref[f] = low
            h = low.astype(jnp.float32)
        else:
            out_ref[f] = h
        mine = h * own_ref[...]
        total = total + jnp.sum(mine.reshape(ROWS // 8, 8, C), axis=0)
        square = square + jnp.sum((mine * h).reshape(ROWS // 8, 8, C), axis=0)
    row = lax.broadcasted_iota(jnp.int32, (8, C), 0)
    total = jnp.sum(total, axis=0, keepdims=True)
    square = jnp.sum(square, axis=0, keepdims=True)
    sums_ref[...] = jnp.where(row == 0, total, jnp.where(row == 1, square, 0.0))


def layer(first, last, h, sums, par, valid, own, weight):
    vmem = pl.BlockSpec(memory_space=pltpu.VMEM)
    return pl.pallas_call(
        functools.partial(layer_kernel, first, last),
        out_shape=(
            jax.ShapeDtypeStruct((FR, ROWS, C), jnp.bfloat16 if last else jnp.float32),
            jax.ShapeDtypeStruct((8, C), jnp.float32),
        ),
        in_specs=[vmem] * 8 + [pl.BlockSpec(memory_space=pl.ANY)],
        out_specs=(vmem, vmem),
        scratch_shapes=[
            pltpu.VMEM((FR, ROWS, 3 * C), jnp.bfloat16),
            pltpu.VMEM((3, 3 * C, C), jnp.bfloat16),
            pltpu.SemaphoreType.DMA,
        ],
        compiler_params=pltpu.CompilerParams(vmem_limit_bytes=24 * 1024 * 1024),
        cost_estimate=pl.CostEstimate(flops=1200000000, bytes_accessed=4000000, transcendentals=300000),
        name="layer",
    )(h, *sums, par, valid, own, weight)


def ordered_kernel(x_ref, out_ref, wide, line):
    for f in range(FR):
        for lane in range(0, C, 128):
            wide[...] = x_ref[f, :, lane : lane + 128].astype(jnp.float32)
            for a in range(STRIPS):
                line[a * SPAN : (a + 1) * SPAN] = wide[pl.ds(a, SPAN, stride=STRIPS)]
            for k in range(4):
                lo = HALO + 64 * k
                out_ref[k, f, :, lane : lane + 128] = line[lo : lo + 64].astype(jnp.bfloat16)


def ordered(x):
    vmem = pl.BlockSpec(memory_space=pltpu.VMEM)
    return pl.pallas_call(
        ordered_kernel,
        out_shape=jax.ShapeDtypeStruct((4, FR, 64, C), jnp.bfloat16),
        in_specs=[vmem],
        out_specs=vmem,
        scratch_shapes=[pltpu.VMEM((ROWS, 128), jnp.float32), pltpu.VMEM((ROWS, 128), jnp.float32)],
        cost_estimate=pl.CostEstimate(flops=2000000, bytes_accessed=2000000, transcendentals=0),
        name="ordered",
    )(x)


def reduced(part):
    chip = part + lax.ppermute(part, "c", [(0, 1), (1, 0)])
    return [chip] + [lax.ppermute(chip, "x", [(i, (i + d) % NX) for i in range(NX)]) for d in (1, 2, 3)]


def in_both_cores(weight, moves):
    core = lax.axis_index("c")
    n = weight.shape[0]
    split = weight.reshape(n, 2, weight.shape[1] // 2, C)
    half = lax.dynamic_index_in_dim(split, core, 1, keepdims=False)
    mine = lax.ppermute(half, "z", moves)
    other = lax.ppermute(mine, "c", [(0, 1), (1, 0)])
    low = jnp.where(core == 0, mine, other)
    high = jnp.where(core == 0, other, mine)
    return jnp.stack([low, high], axis=1).reshape(n, 3, 3 * C, C)


def on_device(clean, noise, timestep, lift, norm_gain, norm_bias, conv_weight, time_proj):
    z, y, x, c = (lax.axis_index(a) for a in ("z", "y", "x", "c"))
    place = 2 * x + c
    own_w = conv_weight[0].reshape(2, 9 * C, C)
    w_near = in_both_cores(own_w, [(2, 1), (6, 7)])
    w_mid = in_both_cores(own_w, [(3, 1), (5, 7)])
    w_far = in_both_cores(own_w[:1], [(4, 7)])
    own_w = own_w.reshape(2, 3, 3 * C, C)

    steps_f = timestep.astype(jnp.float32)
    level = jnp.cos(math.pi / 2.0 * (steps_f / STEPS + 0.008) / 1.008) ** 2
    noisy = jnp.sqrt(level)[:, None, None] * clean + jnp.sqrt(1.0 - level)[:, None, None] * noise
    sent = jnp.broadcast_to(noisy.reshape(NY, 1, FR, 64), (NY, NX * NC, FR, 64)).reshape(NY * NX * NC, FR, 64)
    line = lax.all_to_all(sent, TM, 0, 0, tiled=True)
    line = jnp.pad(line.transpose(1, 0, 2).reshape(FR, -1), ((0, 0), (HALO, HALO)))
    mine = lax.dynamic_slice_in_dim(line, place * OWN, ROWS, axis=1)
    mine = mine.reshape(FR, STRIPS, SPAN).transpose(0, 2, 1).reshape(FR, ROWS)
    h = (mine[..., None] * lift).astype(jnp.bfloat16)

    row = lax.broadcasted_iota(jnp.int32, (ROWS, C), 0)
    frame = (row % STRIPS) * SPAN + row // STRIPS
    when = frame + place * OWN - HALO
    valid = ((when >= 0) & (when < OWN * NX * NC)).astype(jnp.float32)
    own = ((frame >= HALO) & (frame < HALO + OWN)).astype(jnp.float32)
    full = h.astype(jnp.float32) * own
    part = jnp.stack([full.sum(axis=(0, 1)), (full * full).sum(axis=(0, 1))])
    part = jnp.pad(part, ((0, 6), (0, 0)))

    half = C // 2
    freqs = jnp.exp(-math.log(10000.0) * jnp.arange(half, dtype=jnp.float32) / half)
    angles = steps_f[:, None] * freqs[None, :]
    emb = jnp.concatenate([jnp.sin(angles), jnp.cos(angles)], axis=1).astype(jnp.bfloat16)
    temb = jnp.dot(emb, time_proj[0], preferred_element_type=jnp.float32)
    temb = lax.dynamic_slice_in_dim(temb, y, 1, axis=0)
    zero = jnp.zeros((5, C), jnp.float32)
    own_p = jnp.stack([jnp.concatenate([norm_gain[0, i][None], norm_bias[0, i][None], temb, zero]) for i in range(2)])
    p_near = lax.ppermute(own_p, "z", [(2, 1), (6, 7)])
    p_mid = lax.ppermute(own_p, "z", [(3, 1), (5, 7)])
    p_far = lax.ppermute(own_p, "z", [(4, 7)])

    def run(h, part, w, p, depth):
        for i in range(depth):
            h, part = layer(i == 0, i == depth - 1, h, reduced(part), p[i], valid, own, w[i])
        return h, part

    def hop(h, part, moves):
        return lax.ppermute(h, "z", moves), lax.ppermute(part, "z", moves)

    back = []
    h, part = run(h, part, own_w, own_p, 2)
    kept = h
    h, part = hop(h, part, [(0, 1)])
    h, part = run(h, part, own_w, own_p, 2)
    kept = jnp.where(z == 1, h, kept)
    h, part = run(h, part, w_near, p_near, 2)
    back.append((2, lax.ppermute(h, "z", [(1, 2)])))
    h, part = run(h, part, w_mid, p_mid, 2)
    back.append((3, lax.ppermute(h, "z", [(1, 3)])))
    h, part = hop(h, part, [(1, 7)])
    h, part = run(h, part, w_far, p_far, 1)
    back.append((4, lax.ppermute(h, "z", [(7, 4)])))
    h, part = run(h, part, w_mid, p_mid, 1)
    back.append((5, lax.ppermute(h, "z", [(7, 5)])))
    h, part = run(h, part, w_near, p_near, 1)
    back.append((6, lax.ppermute(h, "z", [(7, 6)])))
    h, part = run(h, part, own_w, own_p, 1)
    kept = jnp.where(z == 7, h, kept)
    for at, value in back:
        kept = jnp.where(z == at, value, kept)

    blocks = ordered(kept)
    got = []
    for r in range(NY):
        moves = []
        for m in range(NY):
            k = (m + r) % 4
            for sx in range(NX):
                for sc in range(NC):
                    moves.append(((m * NX + sx) * NC + sc, (sx * NX + 2 * sc + k // 2) * NC + k % 2))
        block = lax.dynamic_index_in_dim(blocks, (y + r) % 4, 0, keepdims=False)
        got.append(lax.ppermute(block, TM, moves))
    at = 2 * (x % 2) + c
    result = jnp.zeros((NY, FR, 64, C), jnp.bfloat16)
    for r in range(NY):
        result = lax.dynamic_update_index_in_dim(result, got[r], (at - r) % 4, 0)
    return result[None]


def solution(mesh):
    grid = Mesh(mesh.devices.reshape(NZ, NY, NX, NC), ("z", "y", "x", "c"))
    in_specs = (
        P(None, None, TM),
        P(None, None, TM),
        P(),
        P(),
        P("z", None, None),
        P("z", None, None),
        P("z", None, None, None, None, None),
        P("z", None, None),
    )
    return jax.shard_map(
        on_device, mesh=grid, in_specs=in_specs, out_specs=P("z", None, None, TM, None), check_vma=False
    )
```

```python
import functools
import math

import jax
import jax.numpy as jnp
from jax import lax
from jax.experimental import pallas as pl
from jax.experimental.pallas import tpu as pltpu
from jax.sharding import Mesh
from jax.sharding import PartitionSpec as P

C = 256
STEPS = 1000
NZ, NY, NX, NC = 8, 4, 4, 2
FR = 4
OWN = 256
HALO = 16
STRIPS = 16
SPAN = (OWN + 2 * HALO) // STRIPS
ROWS = STRIPS * SPAN
POSITIONS = FR * OWN * NY * NC
COUNT = POSITIONS * 8
K = 9 * C
TM = ("y", "x", "c")
ROW = ("y", "c")


def group_total(x):
    lane = lax.broadcasted_iota(jnp.int32, x.shape, 1)
    for step in (1, 2, 4):
        up = pltpu.roll(x, C - step, 1)
        down = pltpu.roll(x, step, 1)
        x = x + jnp.where((lane & step) == 0, up, down)
    return x


def layer_kernel(index, slot, first, last, split, core, h_ref, part_ref, par_ref, valid_ref, own_ref, *refs):
    weights, rest = refs[: 1 + split], refs[1 + split :]
    out_ref, sums_ref = rest[:2]
    act, w_ref, sem = rest[2:]
    if split:
        size = K // 2
        lows = (core[0] * size, (1 - core[0]) * size)
        fetches = [
            pltpu.make_async_copy(w.at[slot], w_ref.at[pl.ds(pl.multiple_of(lo, size), size)], sem.at[n])
            for n, (w, lo) in enumerate(zip(weights, lows))
        ]
    else:
        fetches = [pltpu.make_async_copy(weights[0].at[slot], w_ref, sem.at[0])]
    for fetch in fetches:
        fetch.start()
    sums = jnp.sum(part_ref[...], axis=0)
    total, square = sums[0:1], sums[1:2]
    gain, bias, temb = par_ref[2 * index : 2 * index + 1], par_ref[2 * index + 1 : 2 * index + 2], par_ref[4:5]
    if first:
        square = square + 2.0 * temb * total + POSITIONS * temb * temb
        total = total + POSITIONS * temb
    both = group_total(jnp.concatenate([total, square, jnp.zeros((6, C), jnp.float32)], axis=0))
    mean = both[0:1] / COUNT
    var = both[1:2] / COUNT - mean * mean
    scale = lax.rsqrt(var + 1e-05) * gain

    def activate(f, _):
        for lo in range(0, ROWS, 2 * STRIPS):
            hi = lo + 2 * STRIPS
            h = h_ref[f, lo:hi].astype(jnp.float32)
            if first:
                h = h + temb
            x = (h - mean) * scale + bias
            half = 0.5 * x
            valid = valid_ref[lo:hi]
            a = (half + half * jnp.tanh(half)) * jnp.concatenate([valid, valid], axis=1)
            b = a.astype(jnp.bfloat16)
            act[f, lo:hi, C : 2 * C] = b
            if hi < ROWS:
                act[f, lo + STRIPS : hi + STRIPS, 0:C] = b
            else:
                act[f, hi - STRIPS : hi, 0:C] = b[:STRIPS]
                act[f, 0:STRIPS, 0:C] = pltpu.roll(a[STRIPS:], 1, 0).astype(jnp.bfloat16)
            if lo > 0:
                act[f, lo - STRIPS : hi - STRIPS, 2 * C : 3 * C] = b
            else:
                act[f, 0:STRIPS, 2 * C : 3 * C] = b[STRIPS:]
                act[f, ROWS - STRIPS : ROWS, 2 * C : 3 * C] = pltpu.roll(a[:STRIPS], STRIPS - 1, 0).astype(jnp.bfloat16)
        return 0

    lax.fori_loop(0, FR, activate, 0)
    for fetch in fetches:
        fetch.wait()
    total = jnp.zeros((8, C), jnp.float32)
    square = jnp.zeros((8, C), jnp.float32)
    mine = jnp.concatenate([own_ref[...], own_ref[...]], axis=1)
    for f in range(FR):
        h = h_ref[f].astype(jnp.float32)
        if first:
            h = h + temb
        for i in range(3):
            if 0 <= f + i - 1 < FR:
                h = h + jnp.dot(
                    act[f + i - 1], w_ref[3 * C * i : 3 * C * (i + 1)], preferred_element_type=jnp.float32
                )
        if last:
            low = h.astype(jnp.bfloat16)
            out_ref[f] = low
            h = low.astype(jnp.float32)
        else:
            out_ref[f] = h
        counted = h * mine
        total = total + jnp.sum(counted.reshape(ROWS // 8, 8, C), axis=0)
        square = square + jnp.sum((counted * h).reshape(ROWS // 8, 8, C), axis=0)
    sums = jnp.concatenate([jnp.sum(total, axis=0, keepdims=True), jnp.sum(square, axis=0, keepdims=True)], axis=0)
    for n in range(NY * NC):
        sums_ref[n] = sums


def layer(index, first, last, core, h, part, par, valid, own, weights):
    vmem = pl.BlockSpec(memory_space=pltpu.VMEM)
    hbm = pl.BlockSpec(memory_space=pltpu.HBM)
    out_shape = [
        jax.ShapeDtypeStruct((FR, ROWS, C), jnp.bfloat16 if last else jnp.float32),
        jax.ShapeDtypeStruct((NY * NC, 2, C), jnp.float32),
    ]
    return pl.pallas_call(
        functools.partial(layer_kernel, index, min(index, weights[0].shape[0] - 1), first, last, len(weights) - 1),
        out_shape=tuple(out_shape),
        in_specs=[pl.BlockSpec(memory_space=pltpu.SMEM)] + [vmem] * 5 + [hbm] * len(weights),
        out_specs=(vmem, vmem),
        scratch_shapes=[
            pltpu.VMEM((FR, ROWS, 3 * C), jnp.bfloat16),
            pltpu.VMEM((K, C), jnp.bfloat16),
            pltpu.SemaphoreType.DMA((2,)),
        ],
        compiler_params=pltpu.CompilerParams(vmem_limit_bytes=16 * 1024 * 1024),
        cost_estimate=pl.CostEstimate(flops=1200000000, bytes_accessed=4000000, transcendentals=300000),
        name="layer",
    )(core, h, part, par, valid, own, *weights)


def ordered_kernel(where, *refs):
    sources, (keep_ref, send_ref, x_ref, wide, line, sem) = refs[:NZ], refs[NZ:]
    for z in range(NZ):

        @pl.when(where[0] == z)
        def _():
            copy = pltpu.make_async_copy(sources[z], x_ref, sem)
            copy.start()
            copy.wait()

    core = where[1]
    for f in range(FR):
        for lane in range(0, C, 128):
            wide[...] = x_ref[f, :, lane : lane + 128].astype(jnp.float32)
            for a in range(STRIPS):
                line[a * SPAN : (a + 1) * SPAN] = wide[pl.ds(a, SPAN, stride=STRIPS)]
            for k in range(2):
                lo = pl.multiple_of(HALO + 128 * k + 64 * core, 16)
                keep_ref[k, f, :, lane : lane + 128] = line[pl.ds(lo, 64)].astype(jnp.bfloat16)
                lo = pl.multiple_of(HALO + 128 * k + 64 * (1 - core), 16)
                send_ref[k, f, :, lane : lane + 128] = line[pl.ds(lo, 64)].astype(jnp.bfloat16)


def ordered(where, sources):
    vmem = pl.BlockSpec(memory_space=pltpu.VMEM)
    half = jax.ShapeDtypeStruct((2, FR, 64, C), jnp.bfloat16)
    return pl.pallas_call(
        ordered_kernel,
        out_shape=(half, half),
        in_specs=[pl.BlockSpec(memory_space=pltpu.SMEM)] + [pl.BlockSpec(memory_space=pl.ANY)] * NZ,
        out_specs=(vmem, vmem),
        scratch_shapes=[
            pltpu.VMEM((FR, ROWS, C), jnp.bfloat16),
            pltpu.VMEM((ROWS, 128), jnp.float32),
            pltpu.VMEM((ROWS, 128), jnp.float32),
            pltpu.SemaphoreType.DMA,
        ],
        compiler_params=pltpu.CompilerParams(vmem_limit_bytes=8 * 1024 * 1024),
        cost_estimate=pl.CostEstimate(flops=2000000, bytes_accessed=2000000, transcendentals=0),
        name="ordered",
    )(where, *sources)


def halves_kernel(where, w_hbm, two_hbm, one_hbm, held, sem):
    size = K // 2
    z, core = where[0], where[1]
    rows = pl.ds(pl.multiple_of(core * size, size), size)

    def carry(index, target):
        take = pltpu.make_async_copy(w_hbm.at[index, rows], held.at[index], sem.at[index])
        take.start()
        take.wait()
        give = pltpu.make_async_copy(held.at[index], target.at[index], sem.at[index])
        give.start()
        give.wait()

    @pl.when((z == 2) | (z == 3) | (z == 6))
    def _():
        carry(0, two_hbm)

    @pl.when((z == 2) | (z == 3))
    def _():
        carry(1, two_hbm)

    @pl.when((z == 4) | (z == 5))
    def _():
        carry(0, one_hbm)


def halves(where, weight):
    hbm = pl.BlockSpec(memory_space=pltpu.HBM)
    return pl.pallas_call(
        halves_kernel,
        out_shape=tuple(jax.ShapeDtypeStruct((n, K // 2, C), jnp.bfloat16) for n in (2, 1)),
        in_specs=[pl.BlockSpec(memory_space=pltpu.SMEM), hbm],
        out_specs=(hbm, hbm),
        scratch_shapes=[pltpu.VMEM((2, K // 2, C), jnp.bfloat16), pltpu.SemaphoreType.DMA((2,))],
        compiler_params=pltpu.CompilerParams(vmem_limit_bytes=4 * 1024 * 1024),
        cost_estimate=pl.CostEstimate(flops=1000000, bytes_accessed=5000000, transcendentals=0),
        name="halves",
    )(where, weight)


def moved(value, moves, axis="z"):
    return lax.ppermute(value, axis, moves)


def swapped(value):
    return moved(value, [(0, 1), (1, 0)], "c")


def program(clean, noise, timestep, lift, norm_gain, norm_bias, conv_weight, time_proj):
    z, y, c = (lax.axis_index(a) for a in ("z", "y", "c"))
    place = 2 * y + c
    core = c.reshape(1).astype(jnp.int32)
    own_w = conv_weight[0].reshape(2, K, C)
    where = jnp.stack([z, c]).astype(jnp.int32)
    half, one = halves(where, own_w)
    near = moved(half, [(2, 1), (6, 7)])

    steps_f = timestep.astype(jnp.float32)
    level = jnp.cos(math.pi / 2.0 * (steps_f / STEPS + 0.008) / 1.008) ** 2
    noisy = jnp.sqrt(level)[:, None, None] * clean + jnp.sqrt(1.0 - level)[:, None, None] * noise
    sent = jnp.broadcast_to(noisy[None, :, None], (NY, NX, NC, FR, 64)).reshape(NY * NX * NC, FR * 64)
    lifts = jnp.stack([lift, lift * lift])
    line = lax.all_to_all(sent, TM, 0, 0, tiled=True)
    part = (jnp.stack([line.sum(), (line * line).sum()])[:, None] * lifts)[None]
    line = line.reshape(NY * NX * NC, FR, 64).transpose(1, 0, 2).reshape(FR, -1)
    line = jnp.pad(line, ((0, 0), (HALO, HALO)))
    mine = lax.dynamic_slice_in_dim(line, place * OWN, ROWS, axis=1)
    mine = mine.reshape(FR, STRIPS, SPAN).transpose(0, 2, 1).reshape(FR, ROWS)
    h = (mine[..., None] * lift).astype(jnp.bfloat16)

    row = lax.broadcasted_iota(jnp.int32, (ROWS, 128), 0)
    frame = (row % STRIPS) * SPAN + row // STRIPS
    when = frame + place * OWN - HALO
    valid = ((when >= 0) & (when < OWN * NY * NC)).astype(jnp.float32)
    own = ((frame >= HALO) & (frame < HALO + OWN)).astype(jnp.float32)

    few = C // 2
    freqs = jnp.exp(-math.log(10000.0) * jnp.arange(few, dtype=jnp.float32) / few)
    angles = steps_f[:, None] * freqs[None, :]
    emb = jnp.concatenate([jnp.sin(angles), jnp.cos(angles)], axis=1).astype(jnp.bfloat16)
    temb = jnp.dot(emb, time_proj[0], preferred_element_type=jnp.float32)
    temb = lax.dynamic_slice_in_dim(temb, lax.axis_index("x"), 1, axis=0)
    own_p = jnp.concatenate(
        [norm_gain[0, 0:1], norm_bias[0, 0:1], norm_gain[0, 1:2], norm_bias[0, 1:2], temb, jnp.zeros((3, C), jnp.float32)]
    )
    p3 = moved(own_p, [(3, 1), (5, 7)])
    p4 = moved(own_p, [(4, 1)])
    h, part, valid, own, own_p, p3, p4, where, core = lax.optimization_barrier(
        (h, part, valid, own, own_p, p3, p4, where, core)
    )

    def run(index, last, h, part, p, weights):
        return layer(index, index == 0, last, core, h, part, p, valid, own, weights)

    def stats(part, *settled):
        part, *settled = lax.optimization_barrier((part, *settled))
        part = lax.all_to_all(part, ROW, 0, 0, tiled=True)
        return (part, *settled) if settled else part

    own_w = (own_w,)
    h, part = run(0, False, h, part, own_p, own_w)
    part, half = lax.optimization_barrier((stats(part), half))
    mid = moved(half, [(3, 1)])
    h, part = run(1, True, h, part, own_p, own_w)
    ret0 = h
    part = moved(part, [(0, 1)])
    hopped = moved(h, [(0, 1)])
    part, later_p, one = lax.optimization_barrier((stats(part), own_p, one))
    p2 = moved(later_p, [(2, 1), (6, 7)])
    w4 = moved(one, [(4, 1)])
    w5 = moved(one, [(5, 7)])
    h, part = lax.optimization_barrier((hopped, part))
    h, part = run(0, False, h, part, own_p, own_w)
    part, p2, near = stats(part, p2, near)
    part, near = lax.optimization_barrier((part, near))
    h, part = run(1, True, h, part, own_p, own_w)
    ret1 = h
    nears = swapped(near)
    part, nears = stats(part, nears)
    near = (near, nears)
    h, part = run(0, False, h, part, p2, near)
    part, mid = stats(part, mid)
    part, mid = lax.optimization_barrier((part, mid))
    h, part = run(1, True, h, part, p2, near)
    ret2 = moved(h, [(1, 2)])
    mids = swapped(mid)
    part, mids = stats(part, mids)
    mid = (mid, mids)
    h, part = run(0, False, h, part, p3, mid)
    part, w4 = stats(part, w4)
    part, w4 = lax.optimization_barrier((part, w4))
    h, part = run(1, True, h, part, p3, mid)
    ret3 = moved(h, [(1, 3)])
    w4s = swapped(w4)
    part, w4s, w5 = stats(part, w4s, w5)
    part, w5 = lax.optimization_barrier((part, w5))
    h, part = run(0, True, h, part, p4, (w4, w4s))
    w5s = swapped(w5)
    part, w5s = lax.optimization_barrier((part, w5s))
    part = moved(part, [(1, 7)])
    ret4 = moved(h, [(1, 4)])
    h, part = lax.optimization_barrier((moved(h, [(1, 7)]), stats(part)))
    h, part = run(0, True, h, part, p3, (w5, w5s))
    ret5 = moved(h, [(7, 5)])
    h, part = run(0, True, h, stats(part), p2, near)
    ret6 = moved(h, [(7, 6)])
    h, part = run(0, True, h, stats(part), own_p, own_w)
    ret7 = h

    keep, send = ordered(where, [ret0, ret1, ret2, ret3, ret4, ret5, ret6, ret7])
    got = swapped(send)
    blocks = jnp.where(c == 0, jnp.concatenate([keep, got]), jnp.concatenate([got, keep]))
    return lax.all_to_all(blocks, "x", 0, 0, tiled=True)[None]


def solution(mesh):
    grid = Mesh(mesh.devices.reshape(NZ, NY, NX, NC), ("z", "y", "x", "c"))
    in_specs = (
        P(None, None, TM),
        P(None, None, TM),
        P(),
        P(),
        P("z", None, None),
        P("z", None, None),
        P("z", None, None, None, None, None),
        P("z", None, None),
    )
    return jax.shard_map(program, mesh=grid, in_specs=in_specs, out_specs=P("z", None, None, TM, None), check_vma=False)
```

```python
import functools
import math

import jax
import jax.numpy as jnp
from jax import lax
from jax.experimental import pallas as pl
from jax.experimental.pallas import tpu as pltpu
from jax.sharding import Mesh
from jax.sharding import PartitionSpec as P

C = 256
STEPS = 1000
NZ, NY, NX, NC = 8, 4, 4, 2
FR = 4
OWN = 256
HALO = 16
STRIPS = 16
SPAN = (OWN + 2 * HALO) // STRIPS
ROWS = STRIPS * SPAN
POSITIONS = FR * OWN * NY * NC
COUNT = POSITIONS * 8
K = 9 * C
TM = ("y", "x", "c")
ROW = ("y", "c")


def group_total(x):
    lane = lax.broadcasted_iota(jnp.int32, x.shape, 1)
    for step in (1, 2, 4):
        up = pltpu.roll(x, C - step, 1)
        down = pltpu.roll(x, step, 1)
        x = x + jnp.where((lane & step) == 0, up, down)
    return x


def layer_kernel(index, slot, first, last, split, core, h_ref, part_ref, par_ref, valid_ref, own_ref, *refs):
    weights, rest = refs[: 1 + split], refs[1 + split :]
    out_ref, sums_ref = rest[:2]
    act, w_ref, sem = rest[2:]
    if split:
        size = K // 2
        lows = (core[0] * size, (1 - core[0]) * size)
        fetches = [
            pltpu.make_async_copy(w.at[slot], w_ref.at[pl.ds(pl.multiple_of(lo, size), size)], sem.at[n])
            for n, (w, lo) in enumerate(zip(weights, lows))
        ]
    else:
        fetches = [pltpu.make_async_copy(weights[0].at[slot], w_ref, sem.at[0])]
    for fetch in fetches:
        fetch.start()
    sums = jnp.sum(part_ref[...], axis=0)
    total, square = sums[0:1], sums[1:2]
    gain, bias, temb = par_ref[2 * index : 2 * index + 1], par_ref[2 * index + 1 : 2 * index + 2], par_ref[4:5]
    if first:
        square = square + 2.0 * temb * total + POSITIONS * temb * temb
        total = total + POSITIONS * temb
    both = group_total(jnp.concatenate([total, square, jnp.zeros((6, C), jnp.float32)], axis=0))
    mean = both[0:1] / COUNT
    var = both[1:2] / COUNT - mean * mean
    scale = lax.rsqrt(var + 1e-05) * gain

    def activate(f, _):
        for lo in range(0, ROWS, 2 * STRIPS):
            hi = lo + 2 * STRIPS
            h = h_ref[f, lo:hi].astype(jnp.float32)
            if first:
                h = h + temb
            x = (h - mean) * scale + bias
            half = 0.5 * x
            valid = valid_ref[lo:hi]
            a = (half + half * jnp.tanh(half)) * jnp.concatenate([valid, valid], axis=1)
            b = a.astype(jnp.bfloat16)
            act[f, lo:hi, C : 2 * C] = b
            if hi < ROWS:
                act[f, lo + STRIPS : hi + STRIPS, 0:C] = b
            else:
                act[f, hi - STRIPS : hi, 0:C] = b[:STRIPS]
                act[f, 0:STRIPS, 0:C] = pltpu.roll(a[STRIPS:], 1, 0).astype(jnp.bfloat16)
            if lo > 0:
                act[f, lo - STRIPS : hi - STRIPS, 2 * C : 3 * C] = b
            else:
                act[f, 0:STRIPS, 2 * C : 3 * C] = b[STRIPS:]
                act[f, ROWS - STRIPS : ROWS, 2 * C : 3 * C] = pltpu.roll(a[:STRIPS], STRIPS - 1, 0).astype(jnp.bfloat16)
        return 0

    lax.fori_loop(0, FR, activate, 0)
    for fetch in fetches:
        fetch.wait()
    total = jnp.zeros((8, C), jnp.float32)
    square = jnp.zeros((8, C), jnp.float32)
    mine = jnp.concatenate([own_ref[...], own_ref[...]], axis=1)
    for f in range(FR):
        h = h_ref[f].astype(jnp.float32)
        if first:
            h = h + temb
        for i in range(3):
            if 0 <= f + i - 1 < FR:
                h = h + jnp.dot(
                    act[f + i - 1], w_ref[3 * C * i : 3 * C * (i + 1)], preferred_element_type=jnp.float32
                )
        if last:
            low = h.astype(jnp.bfloat16)
            out_ref[f] = low
            h = low.astype(jnp.float32)
        else:
            out_ref[f] = h
        counted = h * mine
        total = total + jnp.sum(counted.reshape(ROWS // 8, 8, C), axis=0)
        square = square + jnp.sum((counted * h).reshape(ROWS // 8, 8, C), axis=0)
    sums = jnp.concatenate([jnp.sum(total, axis=0, keepdims=True), jnp.sum(square, axis=0, keepdims=True)], axis=0)
    for n in range(NY * NC):
        sums_ref[n] = sums


def layer(index, first, last, core, h, part, par, valid, own, weights):
    vmem = pl.BlockSpec(memory_space=pltpu.VMEM)
    hbm = pl.BlockSpec(memory_space=pltpu.HBM)
    out_shape = [
        jax.ShapeDtypeStruct((FR, ROWS, C), jnp.bfloat16 if last else jnp.float32),
        jax.ShapeDtypeStruct((NY * NC, 2, C), jnp.float32),
    ]
    return pl.pallas_call(
        functools.partial(layer_kernel, index, min(index, weights[0].shape[0] - 1), first, last, len(weights) - 1),
        out_shape=tuple(out_shape),
        in_specs=[pl.BlockSpec(memory_space=pltpu.SMEM)] + [vmem] * 5 + [hbm] * len(weights),
        out_specs=(vmem, vmem),
        scratch_shapes=[
            pltpu.VMEM((FR, ROWS, 3 * C), jnp.bfloat16),
            pltpu.VMEM((K, C), jnp.bfloat16),
            pltpu.SemaphoreType.DMA((2,)),
        ],
        compiler_params=pltpu.CompilerParams(vmem_limit_bytes=16 * 1024 * 1024),
        cost_estimate=pl.CostEstimate(flops=1200000000, bytes_accessed=4000000, transcendentals=300000),
        name="layer",
    )(core, h, part, par, valid, own, *weights)


def ordered_kernel(where, *refs):
    sources, (keep_ref, send_ref, x_ref, wide, line, sem) = refs[:NZ], refs[NZ:]
    for z in range(NZ):

        @pl.when(where[0] == z)
        def _():
            copy = pltpu.make_async_copy(sources[z], x_ref, sem)
            copy.start()
            copy.wait()

    core = where[1]
    for f in range(FR):
        for lane in range(0, C, 128):
            wide[...] = x_ref[f, :, lane : lane + 128].astype(jnp.float32)
            for a in range(STRIPS):
                line[a * SPAN : (a + 1) * SPAN] = wide[pl.ds(a, SPAN, stride=STRIPS)]
            for k in range(2):
                lo = pl.multiple_of(HALO + 128 * k + 64 * core, 16)
                keep_ref[k, f, :, lane : lane + 128] = line[pl.ds(lo, 64)].astype(jnp.bfloat16)
                lo = pl.multiple_of(HALO + 128 * k + 64 * (1 - core), 16)
                send_ref[k, f, :, lane : lane + 128] = line[pl.ds(lo, 64)].astype(jnp.bfloat16)


def ordered(where, sources):
    vmem = pl.BlockSpec(memory_space=pltpu.VMEM)
    half = jax.ShapeDtypeStruct((2, FR, 64, C), jnp.bfloat16)
    return pl.pallas_call(
        ordered_kernel,
        out_shape=(half, half),
        in_specs=[pl.BlockSpec(memory_space=pltpu.SMEM)] + [pl.BlockSpec(memory_space=pl.ANY)] * NZ,
        out_specs=(vmem, vmem),
        scratch_shapes=[
            pltpu.VMEM((FR, ROWS, C), jnp.bfloat16),
            pltpu.VMEM((ROWS, 128), jnp.float32),
            pltpu.VMEM((ROWS, 128), jnp.float32),
            pltpu.SemaphoreType.DMA,
        ],
        compiler_params=pltpu.CompilerParams(vmem_limit_bytes=8 * 1024 * 1024),
        cost_estimate=pl.CostEstimate(flops=2000000, bytes_accessed=2000000, transcendentals=0),
        name="ordered",
    )(where, *sources)


def halves_kernel(where, w_hbm, two_hbm, one_hbm, held, sem):
    size = K // 2
    z, core = where[0], where[1]
    rows = pl.ds(pl.multiple_of(core * size, size), size)

    def carry(index, target):
        take = pltpu.make_async_copy(w_hbm.at[index, rows], held.at[index], sem.at[index])
        take.start()
        take.wait()
        give = pltpu.make_async_copy(held.at[index], target.at[index], sem.at[index])
        give.start()
        give.wait()

    @pl.when((z == 2) | (z == 3) | (z == 6))
    def _():
        carry(0, two_hbm)

    @pl.when((z == 2) | (z == 3))
    def _():
        carry(1, two_hbm)

    @pl.when((z == 4) | (z == 5))
    def _():
        carry(0, one_hbm)


def halves(where, weight):
    hbm = pl.BlockSpec(memory_space=pltpu.HBM)
    return pl.pallas_call(
        halves_kernel,
        out_shape=tuple(jax.ShapeDtypeStruct((n, K // 2, C), jnp.bfloat16) for n in (2, 1)),
        in_specs=[pl.BlockSpec(memory_space=pltpu.SMEM), hbm],
        out_specs=(hbm, hbm),
        scratch_shapes=[pltpu.VMEM((2, K // 2, C), jnp.bfloat16), pltpu.SemaphoreType.DMA((2,))],
        compiler_params=pltpu.CompilerParams(vmem_limit_bytes=60 * 1024 * 1024),
        cost_estimate=pl.CostEstimate(flops=1000000, bytes_accessed=5000000, transcendentals=0),
        name="halves",
    )(where, weight)


def moved(value, moves, axis="z"):
    return lax.ppermute(value, axis, moves)


def swapped(value):
    return moved(value, [(0, 1), (1, 0)], "c")


def program(clean, noise, timestep, lift, norm_gain, norm_bias, conv_weight, time_proj):
    z, y, c = (lax.axis_index(a) for a in ("z", "y", "c"))
    place = 2 * y + c
    core = c.reshape(1).astype(jnp.int32)
    own_w = conv_weight[0].reshape(2, K, C)
    where = jnp.stack([z, c]).astype(jnp.int32)
    half, one = halves(where, own_w)
    near = moved(half, [(2, 1), (6, 7)])

    steps_f = timestep.astype(jnp.float32)
    level = jnp.cos(math.pi / 2.0 * (steps_f / STEPS + 0.008) / 1.008) ** 2
    noisy = jnp.sqrt(level)[:, None, None] * clean + jnp.sqrt(1.0 - level)[:, None, None] * noise
    sent = jnp.broadcast_to(noisy[None, :, None], (NY, NX, NC, FR, 64)).reshape(NY * NX * NC, FR * 64)
    lifts = jnp.stack([lift, lift * lift])
    line = lax.all_to_all(sent, TM, 0, 0, tiled=True)
    part = (jnp.stack([line, line * line]).sum(axis=(1, 2))[:, None] * lifts)[None]
    line = line.reshape(NY * NX * NC, FR, 64).transpose(1, 0, 2).reshape(FR, -1)
    line = jnp.pad(line, ((0, 0), (HALO, HALO)))
    mine = lax.dynamic_slice_in_dim(line, place * OWN, ROWS, axis=1)
    mine = mine.reshape(FR, STRIPS, SPAN).transpose(0, 2, 1).reshape(FR, ROWS)
    h = (mine[..., None] * lift).astype(jnp.bfloat16)

    row = lax.broadcasted_iota(jnp.int32, (ROWS, 128), 0)
    frame = (row % STRIPS) * SPAN + row // STRIPS
    when = frame + place * OWN - HALO
    valid = ((when >= 0) & (when < OWN * NY * NC)).astype(jnp.float32)
    own = ((frame >= HALO) & (frame < HALO + OWN)).astype(jnp.float32)

    few = C // 2
    freqs = jnp.exp(-math.log(10000.0) * jnp.arange(few, dtype=jnp.float32) / few)
    angles = steps_f[:, None] * freqs[None, :]
    emb = jnp.concatenate([jnp.sin(angles), jnp.cos(angles)], axis=1).astype(jnp.bfloat16)
    temb = jnp.dot(emb, time_proj[0], preferred_element_type=jnp.float32)
    temb = lax.dynamic_slice_in_dim(temb, lax.axis_index("x"), 1, axis=0)
    own_p = jnp.concatenate(
        [norm_gain[0, 0:1], norm_bias[0, 0:1], norm_gain[0, 1:2], norm_bias[0, 1:2], temb, jnp.zeros((3, C), jnp.float32)]
    )
    p2 = moved(own_p, [(2, 1), (6, 7)])
    p3 = moved(own_p, [(3, 1), (5, 7)])
    p4 = moved(own_p, [(4, 1)])
    h, part, valid, own, own_p, p2, p3, p4, where, core = lax.optimization_barrier(
        (h, part, valid, own, own_p, p2, p3, p4, where, core)
    )

    def run(index, last, h, part, p, weights):
        return layer(index, index == 0, last, core, h, part, p, valid, own, weights)

    def stats(part, *settled):
        part, *settled = lax.optimization_barrier((part, *settled))
        part = lax.all_to_all(part, ROW, 0, 0, tiled=True)
        return (part, *settled) if settled else part

    own_w = (own_w,)
    h, part = run(0, False, h, part, own_p, own_w)
    h, part = run(1, True, h, stats(part), own_p, own_w)
    ret0 = h
    part = moved(part, [(0, 1)])
    hopped = moved(h, [(0, 1)])
    part, half, one = lax.optimization_barrier((stats(part), half, one))
    mid = moved(half, [(3, 1)])
    w4 = moved(one, [(4, 1)])
    w5 = moved(one, [(5, 7)])
    h, part = lax.optimization_barrier((hopped, part))
    h, part = run(0, False, h, part, own_p, own_w)
    part, near = stats(part, near)
    part, near = lax.optimization_barrier((part, near))
    h, part = run(1, True, h, part, own_p, own_w)
    ret1 = h
    nears = swapped(near)
    part, nears = stats(part, nears)
    near = (near, nears)
    h, part = run(0, False, h, part, p2, near)
    h, part = run(1, True, h, stats(part), p2, near)
    ret2 = moved(h, [(1, 2)])
    mid = (mid, swapped(mid))
    h, part = run(0, False, h, stats(part), p3, mid)
    h, part = run(1, True, h, stats(part), p3, mid)
    ret3 = moved(h, [(1, 3)])
    h, part = run(0, True, h, stats(part), p4, (w4, swapped(w4)))
    w5s = swapped(w5)
    part = moved(part, [(1, 7)])
    ret4 = moved(h, [(1, 4)])
    h, part = lax.optimization_barrier((moved(h, [(1, 7)]), stats(part)))
    h, part = run(0, True, h, part, p3, (w5, w5s))
    ret5 = moved(h, [(7, 5)])
    h, part = run(0, True, h, stats(part), p2, near)
    ret6 = moved(h, [(7, 6)])
    h, part = run(0, True, h, stats(part), own_p, own_w)
    ret7 = h

    keep, send = ordered(where, [ret0, ret1, ret2, ret3, ret4, ret5, ret6, ret7])
    got = swapped(send)
    blocks = jnp.where(c == 0, jnp.concatenate([keep, got]), jnp.concatenate([got, keep]))
    return lax.all_to_all(blocks, "x", 0, 0, tiled=True)[None]


def solution(mesh):
    grid = Mesh(mesh.devices.reshape(NZ, NY, NX, NC), ("z", "y", "x", "c"))
    in_specs = (
        P(None, None, TM),
        P(None, None, TM),
        P(),
        P(),
        P("z", None, None),
        P("z", None, None),
        P("z", None, None, None, None, None),
        P("z", None, None),
    )
    return jax.shard_map(program, mesh=grid, in_specs=in_specs, out_specs=P("z", None, None, TM, None), check_vma=False)
```

```python
import functools
import math

import jax
import jax.numpy as jnp
from jax import lax
from jax.experimental import pallas as pl
from jax.experimental.pallas import tpu as pltpu
from jax.sharding import Mesh
from jax.sharding import PartitionSpec as P

C = 256
STEPS = 1000
NZ, NY, NX, NC = 8, 4, 4, 2
FR = 4
OWN = 256
HALO = 16
STRIPS = 16
SPAN = (OWN + 2 * HALO) // STRIPS
ROWS = STRIPS * SPAN
POSITIONS = FR * OWN * NY * NC
COUNT = POSITIONS * 8
K = 9 * C
TM = ("y", "x", "c")
ROW = ("y", "c")


def group_total(x):
    lane = lax.broadcasted_iota(jnp.int32, x.shape, 1)
    for step in (1, 2, 4):
        up = pltpu.roll(x, C - step, 1)
        down = pltpu.roll(x, step, 1)
        x = x + jnp.where((lane & step) == 0, up, down)
    return x


def layer_kernel(index, slot, base, first, last, split, core, h_ref, part_ref, par_ref, valid_ref, own_ref, *refs):
    weights, rest = refs[: 1 + split], refs[1 + split :]
    out_ref, sums_ref = rest[:2]
    act, w_ref, sem = rest[2:]
    if split:
        size = K // 2
        lows = (core[0] * size, (1 - core[0]) * size)
        fetches = [
            pltpu.make_async_copy(w.at[slot], w_ref.at[pl.ds(pl.multiple_of(lo, size), size)], sem.at[n])
            for n, (w, lo) in enumerate(zip(weights, lows))
        ]
    else:
        fetches = [pltpu.make_async_copy(weights[0].at[slot], w_ref, sem.at[0])]
    for fetch in fetches:
        fetch.start()
    sums = jnp.sum(part_ref[...], axis=0)
    total, square = sums[0:1], sums[1:2]
    gain, bias, temb = (par_ref[base + r : base + r + 1] for r in (2 * index, 2 * index + 1, 4))
    if first:
        square = square + 2.0 * temb * total + POSITIONS * temb * temb
        total = total + POSITIONS * temb
    both = group_total(jnp.concatenate([total, square, jnp.zeros((6, C), jnp.float32)], axis=0))
    mean = both[0:1] / COUNT
    var = both[1:2] / COUNT - mean * mean
    scale = lax.rsqrt(var + 1e-05) * gain

    def activate(f, _):
        for lo in range(0, ROWS, 2 * STRIPS):
            hi = lo + 2 * STRIPS
            h = h_ref[f, lo:hi].astype(jnp.float32)
            if first:
                h = h + temb
            x = (h - mean) * scale + bias
            half = 0.5 * x
            valid = valid_ref[lo:hi]
            a = (half + half * jnp.tanh(half)) * jnp.concatenate([valid, valid], axis=1)
            b = a.astype(jnp.bfloat16)
            act[f, lo:hi, C : 2 * C] = b
            if hi < ROWS:
                act[f, lo + STRIPS : hi + STRIPS, 0:C] = b
            else:
                act[f, hi - STRIPS : hi, 0:C] = b[:STRIPS]
                act[f, 0:STRIPS, 0:C] = pltpu.roll(a[STRIPS:], 1, 0).astype(jnp.bfloat16)
            if lo > 0:
                act[f, lo - STRIPS : hi - STRIPS, 2 * C : 3 * C] = b
            else:
                act[f, 0:STRIPS, 2 * C : 3 * C] = b[STRIPS:]
                act[f, ROWS - STRIPS : ROWS, 2 * C : 3 * C] = pltpu.roll(a[:STRIPS], STRIPS - 1, 0).astype(jnp.bfloat16)
        return 0

    lax.fori_loop(0, FR, activate, 0)
    for fetch in fetches:
        fetch.wait()
    total = jnp.zeros((8, C), jnp.float32)
    square = jnp.zeros((8, C), jnp.float32)
    mine = jnp.concatenate([own_ref[...], own_ref[...]], axis=1)
    for f in range(FR):
        h = h_ref[f].astype(jnp.float32)
        if first:
            h = h + temb
        for i in range(3):
            if 0 <= f + i - 1 < FR:
                h = h + jnp.dot(
                    act[f + i - 1], w_ref[3 * C * i : 3 * C * (i + 1)], preferred_element_type=jnp.float32
                )
        if last:
            low = h.astype(jnp.bfloat16)
            out_ref[f] = low
            h = low.astype(jnp.float32)
        else:
            out_ref[f] = h
        counted = h * mine
        total = total + jnp.sum(counted.reshape(ROWS // 8, 8, C), axis=0)
        square = square + jnp.sum((counted * h).reshape(ROWS // 8, 8, C), axis=0)
    sums = jnp.concatenate([jnp.sum(total, axis=0, keepdims=True), jnp.sum(square, axis=0, keepdims=True)], axis=0)
    for n in range(NY * NC):
        sums_ref[n] = sums


def layer(index, base, first, last, core, h, part, par, valid, own, weights):
    vmem = pl.BlockSpec(memory_space=pltpu.VMEM)
    hbm = pl.BlockSpec(memory_space=pltpu.HBM)
    out_shape = [
        jax.ShapeDtypeStruct((FR, ROWS, C), jnp.bfloat16 if last else jnp.float32),
        jax.ShapeDtypeStruct((NY * NC, 2, C), jnp.float32),
    ]
    return pl.pallas_call(
        functools.partial(layer_kernel, index, min(index, weights[0].shape[0] - 1), base, first, last, len(weights) - 1),
        out_shape=tuple(out_shape),
        in_specs=[pl.BlockSpec(memory_space=pltpu.SMEM)] + [vmem] * 5 + [hbm] * len(weights),
        out_specs=(vmem, vmem),
        scratch_shapes=[
            pltpu.VMEM((FR, ROWS, 3 * C), jnp.bfloat16),
            pltpu.VMEM((K, C), jnp.bfloat16),
            pltpu.SemaphoreType.DMA((2,)),
        ],
        compiler_params=pltpu.CompilerParams(vmem_limit_bytes=16 * 1024 * 1024),
        cost_estimate=pl.CostEstimate(flops=1200000000, bytes_accessed=4000000, transcendentals=300000),
        name="layer",
    )(core, h, part, par, valid, own, *weights)


def ordered_kernel(plane, half, *refs):
    sources, (keep_ref, send_ref, x_ref, wide, line, sem) = refs[:NZ], refs[NZ:]
    for z in range(NZ):

        @pl.when(plane[0] == z)
        def _():
            copy = pltpu.make_async_copy(sources[z], x_ref, sem)
            copy.start()
            copy.wait()

    core = half[0]
    for f in range(FR):
        for lane in range(0, C, 128):
            wide[...] = x_ref[f, :, lane : lane + 128].astype(jnp.float32)
            for a in range(STRIPS):
                line[a * SPAN : (a + 1) * SPAN] = wide[pl.ds(a, SPAN, stride=STRIPS)]
            for k in range(2):
                lo = pl.multiple_of(HALO + 128 * k + 64 * core, 16)
                keep_ref[k, f, :, lane : lane + 128] = line[pl.ds(lo, 64)].astype(jnp.bfloat16)
                lo = pl.multiple_of(HALO + 128 * k + 64 * (1 - core), 16)
                send_ref[k, f, :, lane : lane + 128] = line[pl.ds(lo, 64)].astype(jnp.bfloat16)


def ordered(plane, core, sources):
    vmem = pl.BlockSpec(memory_space=pltpu.VMEM)
    half = jax.ShapeDtypeStruct((2, FR, 64, C), jnp.bfloat16)
    return pl.pallas_call(
        ordered_kernel,
        out_shape=(half, half),
        in_specs=[pl.BlockSpec(memory_space=pltpu.SMEM)] * 2 + [pl.BlockSpec(memory_space=pl.ANY)] * NZ,
        out_specs=(vmem, vmem),
        scratch_shapes=[
            pltpu.VMEM((FR, ROWS, C), jnp.bfloat16),
            pltpu.VMEM((ROWS, 128), jnp.float32),
            pltpu.VMEM((ROWS, 128), jnp.float32),
            pltpu.SemaphoreType.DMA,
        ],
        compiler_params=pltpu.CompilerParams(vmem_limit_bytes=8 * 1024 * 1024),
        cost_estimate=pl.CostEstimate(flops=2000000, bytes_accessed=2000000, transcendentals=0),
        name="ordered",
    )(plane, core, *sources)


def halves_kernel(plane, half, w_hbm, two_hbm, one_hbm, held, sem):
    size = K // 2
    z, core = plane[0], half[0]
    rows = pl.ds(pl.multiple_of(core * size, size), size)

    def carry(layers, target):
        takes = [pltpu.make_async_copy(w_hbm.at[i, rows], held.at[i], sem.at[i]) for i in range(layers)]
        gives = [pltpu.make_async_copy(held.at[i], target.at[i], sem.at[2 + i]) for i in range(layers)]
        for take in takes:
            take.start()
        for take, give in zip(takes, gives):
            take.wait()
            give.start()
        for give in gives:
            give.wait()

    @pl.when((z == 2) | (z == 3))
    def _():
        carry(2, two_hbm)

    @pl.when(z == 6)
    def _():
        carry(1, two_hbm)

    @pl.when((z == 4) | (z == 5))
    def _():
        carry(1, one_hbm)


def halves(plane, core, weight):
    hbm = pl.BlockSpec(memory_space=pltpu.HBM)
    return pl.pallas_call(
        halves_kernel,
        out_shape=tuple(jax.ShapeDtypeStruct((n, K // 2, C), jnp.bfloat16) for n in (2, 1)),
        in_specs=[pl.BlockSpec(memory_space=pltpu.SMEM)] * 2 + [hbm],
        out_specs=(hbm, hbm),
        scratch_shapes=[pltpu.VMEM((2, K // 2, C), jnp.bfloat16), pltpu.SemaphoreType.DMA((4,))],
        compiler_params=pltpu.CompilerParams(vmem_limit_bytes=60 * 1024 * 1024),
        cost_estimate=pl.CostEstimate(flops=1000000, bytes_accessed=5000000, transcendentals=0),
        name="halves",
    )(plane, core, weight)


def moved(value, moves, axis="z"):
    return lax.ppermute(value, axis, moves)


def swapped(value):
    return moved(value, [(0, 1), (1, 0)], "c")


def program(clean, noise, timestep, lift, norm_gain, norm_bias, conv_weight, time_proj):
    z, y, c = (lax.axis_index(a) for a in ("z", "y", "c"))
    place = 2 * y + c
    core = c.reshape(1).astype(jnp.int32)
    own_w = conv_weight[0].reshape(2, K, C)
    plane = z.reshape(1).astype(jnp.int32)
    half, one = halves(plane, core, own_w)
    near = moved(half, [(2, 1), (6, 7)])

    steps_f = timestep.astype(jnp.float32)
    level = jnp.cos(math.pi / 2.0 * (steps_f / STEPS + 0.008) / 1.008) ** 2
    noisy = jnp.sqrt(level)[:, None, None] * clean + jnp.sqrt(1.0 - level)[:, None, None] * noise
    sent = jnp.broadcast_to(noisy[None, :, None], (NY, NX, NC, FR, 64)).reshape(NY * NX * NC, FR * 64)
    lifts = jnp.stack([lift, lift * lift])
    line = lax.all_to_all(sent, TM, 0, 0, tiled=True)
    part = (jnp.stack([line, line * line]).sum(axis=(1, 2))[:, None] * lifts)[None]
    line = line.reshape(NY * NX * NC, FR, 64).transpose(1, 0, 2).reshape(FR, -1)
    line = jnp.pad(line, ((0, 0), (HALO, HALO)))
    mine = lax.dynamic_slice_in_dim(line, place * OWN, ROWS, axis=1)
    mine = mine.reshape(FR, STRIPS, SPAN).transpose(0, 2, 1).reshape(FR, ROWS)
    h = (mine[..., None] * lift).astype(jnp.bfloat16)

    row = lax.broadcasted_iota(jnp.int32, (ROWS, 128), 0)
    frame = (row % STRIPS) * SPAN + row // STRIPS
    when = frame + place * OWN - HALO
    valid = ((when >= 0) & (when < OWN * NY * NC)).astype(jnp.float32)
    own = ((frame >= HALO) & (frame < HALO + OWN)).astype(jnp.float32)

    few = C // 2
    freqs = jnp.exp(-math.log(10000.0) * jnp.arange(few, dtype=jnp.float32) / few)
    angles = steps_f[:, None] * freqs[None, :]
    emb = jnp.concatenate([jnp.sin(angles), jnp.cos(angles)], axis=1).astype(jnp.bfloat16)
    temb = jnp.dot(emb, time_proj[0], preferred_element_type=jnp.float32)
    temb = lax.dynamic_slice_in_dim(temb, lax.axis_index("x"), 1, axis=0)
    own_p = jnp.concatenate(
        [norm_gain[0, 0:1], norm_bias[0, 0:1], norm_gain[0, 1:2], norm_bias[0, 1:2], temb, jnp.zeros((3, C), jnp.float32)]
    )
    p2 = moved(own_p, [(2, 1), (6, 7), (4, 3)])
    h, part, valid, own, own_p, core = lax.optimization_barrier((h, part, valid, own, own_p, core))

    def run(index, last, h, part, p, weights, base=0):
        return layer(index, base, index == 0, last, core, h, part, p, valid, own, weights)

    def stats(part, *settled):
        part, *settled = lax.optimization_barrier((part, *settled))
        part = lax.all_to_all(part, ROW, 0, 0, tiled=True)
        return (part, *settled) if settled else part

    own_w = (own_w,)
    h, part = run(0, False, h, part, own_p, own_w)
    h, part = run(1, True, h, stats(part), own_p, own_w)
    ret0 = h
    hopped = moved(h, [(0, 1)])
    part, p2 = stats(part, p2)
    part, half, sent_p = lax.optimization_barrier((part, half, own_p))
    part = moved(part, [(0, 1)])
    p3 = moved(jnp.concatenate([sent_p, p2]), [(3, 1), (5, 7)])
    mid = moved(half, [(3, 1)])
    h, part = lax.optimization_barrier((hopped, part))
    h, part = run(0, False, h, part, own_p, own_w)
    h, part = run(1, True, h, stats(part), own_p, own_w)
    ret1 = h
    near = (near, swapped(near))
    part = stats(part)
    part, one = lax.optimization_barrier((part, one))
    w4 = moved(one, [(4, 1)])
    w5 = moved(one, [(5, 7)])
    h, part = run(0, False, h, part, p2, near)
    h, part = run(1, True, h, stats(part), p2, near)
    ret2 = moved(h, [(1, 2)])
    mid = (mid, swapped(mid))
    part, p3 = stats(part, p3)
    h, part = run(0, False, h, part, p3, mid)
    h, part = run(1, True, h, stats(part), p3, mid)
    ret3 = moved(h, [(1, 3)])
    h, part = run(0, True, h, stats(part), p3, (w4, swapped(w4)), 8)
    w5s = swapped(w5)
    hopped = moved(h, [(1, 7)])
    part = moved(stats(part), [(1, 7)])
    ret4 = moved(h, [(1, 4)])
    h, part = lax.optimization_barrier((hopped, part))
    h, part = run(0, True, h, part, p3, (w5, w5s))
    ret5 = moved(h, [(7, 5)])
    h, part = run(0, True, h, stats(part), p2, near)
    ret6 = moved(h, [(7, 6)])
    h, part = run(0, True, h, stats(part), own_p, own_w)
    ret7 = h

    keep, send = ordered(plane, core, [ret0, ret1, ret2, ret3, ret4, ret5, ret6, ret7])
    got = swapped(send)
    blocks = jnp.where(c == 0, jnp.concatenate([keep, got]), jnp.concatenate([got, keep]))
    return lax.all_to_all(blocks, "x", 0, 0, tiled=True)[None]


def solution(mesh):
    grid = Mesh(mesh.devices.reshape(NZ, NY, NX, NC), ("z", "y", "x", "c"))
    in_specs = (
        P(None, None, TM),
        P(None, None, TM),
        P(),
        P(),
        P("z", None, None),
        P("z", None, None),
        P("z", None, None, None, None, None),
        P("z", None, None),
    )
    return jax.shard_map(program, mesh=grid, in_specs=in_specs, out_specs=P("z", None, None, TM, None), check_vma=False)
```

```python
import functools
import math

import jax
import jax.numpy as jnp
from jax import lax
from jax.experimental import pallas as pl
from jax.experimental.pallas import tpu as pltpu
from jax.sharding import Mesh
from jax.sharding import PartitionSpec as P

C = 256
STEPS = 1000
NZ, NY, NX, NC = 8, 4, 4, 2
FR = 4
OWN = 256
HALO = 16
STRIPS = 16
SPAN = (OWN + 2 * HALO) // STRIPS
ROWS = STRIPS * SPAN
POSITIONS = FR * OWN * NY * NC
COUNT = POSITIONS * 8
K = 9 * C
TM = ("y", "x", "c")
ROW = ("y", "c")


def group_total(x):
    lane = lax.broadcasted_iota(jnp.int32, x.shape, 1)
    for step in (1, 2, 4):
        up = pltpu.roll(x, C - step, 1)
        down = pltpu.roll(x, step, 1)
        x = x + jnp.where((lane & step) == 0, up, down)
    return x


def layer_kernel(index, slot, base, first, last, split, core, h_ref, part_ref, par_ref, valid_ref, own_ref, *refs):
    weights, rest = refs[: 1 + split], refs[1 + split :]
    out_ref, sums_ref = rest[:2]
    act, w_ref, sem = rest[2:]
    if split:
        size = K // 2
        lows = (core[0] * size, (1 - core[0]) * size)
        fetches = [
            pltpu.make_async_copy(w.at[slot], w_ref.at[pl.ds(pl.multiple_of(lo, size), size)], sem.at[n])
            for n, (w, lo) in enumerate(zip(weights, lows))
        ]
    else:
        fetches = [pltpu.make_async_copy(weights[0].at[slot], w_ref, sem.at[0])]
    for fetch in fetches:
        fetch.start()
    sums = jnp.sum(part_ref[...], axis=0)
    total, square = sums[0:1], sums[1:2]
    gain, bias, temb = (par_ref[base + r : base + r + 1] for r in (2 * index, 2 * index + 1, 4))
    if first:
        square = square + 2.0 * temb * total + POSITIONS * temb * temb
        total = total + POSITIONS * temb
    both = group_total(jnp.concatenate([total, square, jnp.zeros((6, C), jnp.float32)], axis=0))
    mean = both[0:1] / COUNT
    var = both[1:2] / COUNT - mean * mean
    scale = 0.5 * lax.rsqrt(var + 1e-05) * gain
    shift = 0.5 * bias
    centre = mean - temb if first else mean

    def activate(f, _):
        for lo in range(0, ROWS, 2 * STRIPS):
            hi = lo + 2 * STRIPS
            h = h_ref[f, lo:hi].astype(jnp.float32)
            half = (h - centre) * scale + shift
            valid = valid_ref[lo:hi]
            a = (half + half * jnp.tanh(half)) * jnp.concatenate([valid, valid], axis=1)
            b = a.astype(jnp.bfloat16)
            act[f, lo:hi, C : 2 * C] = b
            if hi < ROWS:
                act[f, lo + STRIPS : hi + STRIPS, 0:C] = b
            else:
                act[f, hi - STRIPS : hi, 0:C] = b[:STRIPS]
                act[f, 0:STRIPS, 0:C] = pltpu.roll(a[STRIPS:], 1, 0).astype(jnp.bfloat16)
            if lo > 0:
                act[f, lo - STRIPS : hi - STRIPS, 2 * C : 3 * C] = b
            else:
                act[f, 0:STRIPS, 2 * C : 3 * C] = b[STRIPS:]
                act[f, ROWS - STRIPS : ROWS, 2 * C : 3 * C] = pltpu.roll(a[:STRIPS], STRIPS - 1, 0).astype(jnp.bfloat16)
        return 0

    lax.fori_loop(0, FR, activate, 0)
    for fetch in fetches:
        fetch.wait()
    total = jnp.zeros((8, C), jnp.float32)
    square = jnp.zeros((8, C), jnp.float32)
    mine = jnp.concatenate([own_ref[...], own_ref[...]], axis=1)
    for f in range(FR):
        h = h_ref[f].astype(jnp.float32)
        if first:
            h = h + temb
        for i in range(3):
            if 0 <= f + i - 1 < FR:
                h = h + jnp.dot(
                    act[f + i - 1], w_ref[3 * C * i : 3 * C * (i + 1)], preferred_element_type=jnp.float32
                )
        if last:
            low = h.astype(jnp.bfloat16)
            out_ref[f] = low
            h = low.astype(jnp.float32)
        else:
            out_ref[f] = h
        counted = h * mine
        total = total + jnp.sum(counted.reshape(ROWS // 8, 8, C), axis=0)
        square = square + jnp.sum((counted * h).reshape(ROWS // 8, 8, C), axis=0)
    sums = jnp.concatenate([jnp.sum(total, axis=0, keepdims=True), jnp.sum(square, axis=0, keepdims=True)], axis=0)
    for n in range(NY * NC):
        sums_ref[n] = sums


def layer(index, base, first, last, core, h, part, par, valid, own, weights):
    vmem = pl.BlockSpec(memory_space=pltpu.VMEM)
    hbm = pl.BlockSpec(memory_space=pltpu.HBM)
    out_shape = [
        jax.ShapeDtypeStruct((FR, ROWS, C), jnp.bfloat16 if last else jnp.float32),
        jax.ShapeDtypeStruct((NY * NC, 2, C), jnp.float32),
    ]
    return pl.pallas_call(
        functools.partial(layer_kernel, index, min(index, weights[0].shape[0] - 1), base, first, last, len(weights) - 1),
        out_shape=tuple(out_shape),
        in_specs=[pl.BlockSpec(memory_space=pltpu.SMEM)] + [vmem] * 5 + [hbm] * len(weights),
        out_specs=(vmem, vmem),
        scratch_shapes=[
            pltpu.VMEM((FR, ROWS, 3 * C), jnp.bfloat16),
            pltpu.VMEM((K, C), jnp.bfloat16),
            pltpu.SemaphoreType.DMA((2,)),
        ],
        compiler_params=pltpu.CompilerParams(vmem_limit_bytes=16 * 1024 * 1024),
        cost_estimate=pl.CostEstimate(flops=1200000000, bytes_accessed=4000000, transcendentals=300000),
        name="layer",
    )(core, h, part, par, valid, own, *weights)


def ordered_kernel(plane, half, *refs):
    sources, (keep_ref, send_ref, x_ref, wide, line, sem) = refs[:NZ], refs[NZ:]
    for z in range(NZ):

        @pl.when(plane[0] == z)
        def _():
            copy = pltpu.make_async_copy(sources[z], x_ref, sem)
            copy.start()
            copy.wait()

    core = half[0]
    for f in range(FR):
        for lane in range(0, C, 128):
            wide[...] = x_ref[f, :, lane : lane + 128].astype(jnp.float32)
            for a in range(STRIPS):
                line[a * SPAN : (a + 1) * SPAN] = wide[pl.ds(a, SPAN, stride=STRIPS)]
            for k in range(2):
                lo = pl.multiple_of(HALO + 128 * k + 64 * core, 16)
                keep_ref[k, f, :, lane : lane + 128] = line[pl.ds(lo, 64)].astype(jnp.bfloat16)
                lo = pl.multiple_of(HALO + 128 * k + 64 * (1 - core), 16)
                send_ref[k, f, :, lane : lane + 128] = line[pl.ds(lo, 64)].astype(jnp.bfloat16)


def ordered(plane, core, sources):
    vmem = pl.BlockSpec(memory_space=pltpu.VMEM)
    half = jax.ShapeDtypeStruct((2, FR, 64, C), jnp.bfloat16)
    return pl.pallas_call(
        ordered_kernel,
        out_shape=(half, half),
        in_specs=[pl.BlockSpec(memory_space=pltpu.SMEM)] * 2 + [pl.BlockSpec(memory_space=pl.ANY)] * NZ,
        out_specs=(vmem, vmem),
        scratch_shapes=[
            pltpu.VMEM((FR, ROWS, C), jnp.bfloat16),
            pltpu.VMEM((ROWS, 128), jnp.float32),
            pltpu.VMEM((ROWS, 128), jnp.float32),
            pltpu.SemaphoreType.DMA,
        ],
        compiler_params=pltpu.CompilerParams(vmem_limit_bytes=8 * 1024 * 1024),
        cost_estimate=pl.CostEstimate(flops=2000000, bytes_accessed=2000000, transcendentals=0),
        name="ordered",
    )(plane, core, *sources)


def halves_kernel(plane, half, w_hbm, two_hbm, one_hbm, held, sem):
    size = K // 2
    z, core = plane[0], half[0]
    rows = pl.ds(pl.multiple_of(core * size, size), size)

    def carry(layers, target):
        takes = [pltpu.make_async_copy(w_hbm.at[i, rows], held.at[i], sem.at[i]) for i in range(layers)]
        gives = [pltpu.make_async_copy(held.at[i], target.at[i], sem.at[2 + i]) for i in range(layers)]
        for take in takes:
            take.start()
        for take, give in zip(takes, gives):
            take.wait()
            give.start()
        for give in gives:
            give.wait()

    @pl.when((z == 2) | (z == 3))
    def _():
        carry(2, two_hbm)

    @pl.when((z == 4) | (z == 5) | (z == 6))
    def _():
        carry(1, one_hbm)


def halves(plane, core, weight):
    hbm = pl.BlockSpec(memory_space=pltpu.HBM)
    return pl.pallas_call(
        halves_kernel,
        out_shape=tuple(jax.ShapeDtypeStruct((n, K // 2, C), jnp.bfloat16) for n in (2, 1)),
        in_specs=[pl.BlockSpec(memory_space=pltpu.SMEM)] * 2 + [hbm],
        out_specs=(hbm, hbm),
        scratch_shapes=[pltpu.VMEM((2, K // 2, C), jnp.bfloat16), pltpu.SemaphoreType.DMA((4,))],
        compiler_params=pltpu.CompilerParams(vmem_limit_bytes=60 * 1024 * 1024),
        cost_estimate=pl.CostEstimate(flops=1000000, bytes_accessed=5000000, transcendentals=0),
        name="halves",
    )(plane, core, weight)


def moved(value, moves, axis="z"):
    return lax.ppermute(value, axis, moves)


def swapped(value):
    return moved(value, [(0, 1), (1, 0)], "c")


def program(clean, noise, timestep, lift, norm_gain, norm_bias, conv_weight, time_proj):
    z, y, c = (lax.axis_index(a) for a in ("z", "y", "c"))
    place = 2 * y + c
    core = c.reshape(1).astype(jnp.int32)
    own_w = conv_weight[0].reshape(2, K, C)
    plane = z.reshape(1).astype(jnp.int32)
    half, one = halves(plane, core, own_w)
    near = moved(half, [(2, 1)])

    steps_f = timestep.astype(jnp.float32)
    level = jnp.cos(math.pi / 2.0 * (steps_f / STEPS + 0.008) / 1.008) ** 2
    noisy = jnp.sqrt(level)[:, None, None] * clean + jnp.sqrt(1.0 - level)[:, None, None] * noise
    sent = jnp.broadcast_to(noisy[None, :, None], (NY, NX, NC, FR, 64)).reshape(NY * NX * NC, FR * 64)
    lifts = jnp.stack([lift, lift * lift])
    line = lax.all_to_all(sent, TM, 0, 0, tiled=True)
    part = (jnp.stack([line, line * line]).sum(axis=(1, 2))[:, None] * lifts)[None]
    line = line.reshape(NY * NX * NC, FR, 64).transpose(1, 0, 2).reshape(FR, -1)
    line = jnp.pad(line, ((0, 0), (HALO, HALO)))
    mine = lax.dynamic_slice_in_dim(line, place * OWN, ROWS, axis=1)
    mine = mine.reshape(FR, STRIPS, SPAN).transpose(0, 2, 1).reshape(FR, ROWS)
    h = (mine[..., None] * lift).astype(jnp.bfloat16)

    row = lax.broadcasted_iota(jnp.int32, (ROWS, 128), 0)
    frame = (row % STRIPS) * SPAN + row // STRIPS
    when = frame + place * OWN - HALO
    valid = ((when >= 0) & (when < OWN * NY * NC)).astype(jnp.float32)
    own = ((frame >= HALO) & (frame < HALO + OWN)).astype(jnp.float32)

    few = C // 2
    freqs = jnp.exp(-math.log(10000.0) * jnp.arange(few, dtype=jnp.float32) / few)
    angles = steps_f[:, None] * freqs[None, :]
    emb = jnp.concatenate([jnp.sin(angles), jnp.cos(angles)], axis=1).astype(jnp.bfloat16)
    temb = jnp.dot(emb, time_proj[0], preferred_element_type=jnp.float32)
    temb = lax.dynamic_slice_in_dim(temb, lax.axis_index("x"), 1, axis=0)
    own_p = jnp.concatenate(
        [norm_gain[0, 0:1], norm_bias[0, 0:1], norm_gain[0, 1:2], norm_bias[0, 1:2], temb, jnp.zeros((3, C), jnp.float32)]
    )
    p2 = moved(own_p, [(2, 1), (6, 7), (4, 3)])
    h, part, valid, own, own_p, core = lax.optimization_barrier((h, part, valid, own, own_p, core))

    def run(index, last, h, part, p, weights, base=0):
        return layer(index, base, index == 0, last, core, h, part, p, valid, own, weights)

    def stats(part, *settled):
        part, *settled = lax.optimization_barrier((part, *settled))
        part = lax.all_to_all(part, ROW, 0, 0, tiled=True)
        return (part, *settled) if settled else part

    own_w = (own_w,)
    h, part = run(0, False, h, part, own_p, own_w)
    h, part = run(1, True, h, stats(part), own_p, own_w)
    ret0 = h
    hopped = moved(h, [(0, 1)])
    part, p2 = stats(part, p2)
    part, half, one, sent_p = lax.optimization_barrier((part, half, one, own_p))
    part = moved(part, [(0, 1)])
    p3 = moved(jnp.concatenate([sent_p, p2]), [(3, 1), (5, 7)])
    mid = moved(half, [(3, 1)])
    w46 = moved(one, [(4, 1), (6, 7)])
    w5 = moved(one, [(5, 7)])
    h, part = lax.optimization_barrier((hopped, part))
    h, part = run(0, False, h, part, own_p, own_w)
    h, part = run(1, True, h, stats(part), own_p, own_w)
    ret1 = h
    near = (near, swapped(near))
    h, part = run(0, False, h, stats(part), p2, near)
    h, part = run(1, True, h, stats(part), p2, near)
    ret2 = moved(h, [(1, 2)])
    mid = (mid, swapped(mid))
    part, p3 = stats(part, p3)
    h, part = run(0, False, h, part, p3, mid)
    h, part = run(1, True, h, stats(part), p3, mid)
    back3 = h
    w46 = (w46, swapped(w46))
    h, part = run(0, True, h, stats(part), p3, w46, 8)
    w5s = swapped(w5)
    hopped = moved(h, [(1, 7)])
    part = moved(stats(part), [(1, 7)])
    ret3 = moved(back3, [(1, 3)])
    ret4 = moved(h, [(1, 4)])
    h, part = lax.optimization_barrier((hopped, part))
    h, part = run(0, True, h, part, p3, (w5, w5s))
    ret5 = moved(h, [(7, 5)])
    h, part = run(0, True, h, stats(part), p2, w46)
    ret6 = moved(h, [(7, 6)])
    h, part = run(0, True, h, stats(part), own_p, own_w)
    ret7 = h

    keep, send = ordered(plane, core, [ret0, ret1, ret2, ret3, ret4, ret5, ret6, ret7])
    got = swapped(send)
    blocks = jnp.where(c == 0, jnp.concatenate([keep, got]), jnp.concatenate([got, keep]))
    return lax.all_to_all(blocks, "x", 0, 0, tiled=True)[None]


def solution(mesh):
    grid = Mesh(mesh.devices.reshape(NZ, NY, NX, NC), ("z", "y", "x", "c"))
    in_specs = (
        P(None, None, TM),
        P(None, None, TM),
        P(),
        P(),
        P("z", None, None),
        P("z", None, None),
        P("z", None, None, None, None, None),
        P("z", None, None),
    )
    return jax.shard_map(program, mesh=grid, in_specs=in_specs, out_specs=P("z", None, None, TM, None), check_vma=False)
```

```python
import functools
import math

import jax
import jax.numpy as jnp
from jax import lax
from jax.experimental import pallas as pl
from jax.experimental.pallas import tpu as pltpu
from jax.sharding import Mesh
from jax.sharding import PartitionSpec as P

C = 256
STEPS = 1000
NZ, NY, NX, NC = 8, 4, 4, 2
FR = 4
OWN = 256
HALO = 16
STRIPS = 16
SPAN = (OWN + 2 * HALO) // STRIPS
ROWS = STRIPS * SPAN
POSITIONS = FR * OWN * NY * NC
COUNT = POSITIONS * 8
K = 9 * C
TM = ("y", "x", "c")
ROW = ("y", "c")


def group_total(x):
    lane = lax.broadcasted_iota(jnp.int32, x.shape, 1)
    for step in (1, 2, 4):
        up = pltpu.roll(x, C - step, 1)
        down = pltpu.roll(x, step, 1)
        x = x + jnp.where((lane & step) == 0, up, down)
    return x


def layer_kernel(index, slot, base, first, last, split, core, h_ref, part_ref, par_ref, valid_ref, own_ref, *refs):
    weights, rest = refs[: 1 + split], refs[1 + split :]
    out_ref, sums_ref = rest[:2]
    act, w_ref, sem = rest[2:]
    if split:
        size = K // 2
        lows = (core[0] * size, (1 - core[0]) * size)
        fetches = [
            pltpu.make_async_copy(w.at[slot], w_ref.at[pl.ds(pl.multiple_of(lo, size), size)], sem.at[n])
            for n, (w, lo) in enumerate(zip(weights, lows))
        ]
    else:
        fetches = [pltpu.make_async_copy(weights[0].at[slot], w_ref, sem.at[0])]
    for fetch in fetches:
        fetch.start()
    sums = jnp.sum(part_ref[...], axis=0)
    total, square = sums[0:1], sums[1:2]
    gain, bias, temb = (par_ref[base + r : base + r + 1] for r in (2 * index, 2 * index + 1, 4))
    if first:
        square = square + 2.0 * temb * total + POSITIONS * temb * temb
        total = total + POSITIONS * temb
    both = group_total(jnp.concatenate([total, square, jnp.zeros((6, C), jnp.float32)], axis=0))
    mean = both[0:1] / COUNT
    var = both[1:2] / COUNT - mean * mean
    scale = 0.5 * lax.rsqrt(var + 1e-05) * gain
    shift = 0.5 * bias
    centre = mean - temb if first else mean

    def activate(f, _):
        for lo in range(0, ROWS, 2 * STRIPS):
            hi = lo + 2 * STRIPS
            h = h_ref[f, lo:hi].astype(jnp.float32)
            half = (h - centre) * scale + shift
            valid = valid_ref[lo:hi]
            a = (half + half * jnp.tanh(half)) * jnp.concatenate([valid, valid], axis=1)
            b = a.astype(jnp.bfloat16)
            act[f, lo:hi, C : 2 * C] = b
            if hi < ROWS:
                act[f, lo + STRIPS : hi + STRIPS, 0:C] = b
            else:
                act[f, hi - STRIPS : hi, 0:C] = b[:STRIPS]
                act[f, 0:STRIPS, 0:C] = pltpu.roll(a[STRIPS:], 1, 0).astype(jnp.bfloat16)
            if lo > 0:
                act[f, lo - STRIPS : hi - STRIPS, 2 * C : 3 * C] = b
            else:
                act[f, 0:STRIPS, 2 * C : 3 * C] = b[STRIPS:]
                act[f, ROWS - STRIPS : ROWS, 2 * C : 3 * C] = pltpu.roll(a[:STRIPS], STRIPS - 1, 0).astype(jnp.bfloat16)
        return 0

    lax.fori_loop(0, FR, activate, 0)
    for fetch in fetches:
        fetch.wait()
    total = jnp.zeros((8, C), jnp.float32)
    square = jnp.zeros((8, C), jnp.float32)
    mine = jnp.concatenate([own_ref[...], own_ref[...]], axis=1)
    for f in range(FR):
        h = h_ref[f].astype(jnp.float32)
        if first:
            h = h + temb
        for i in range(3):
            if 0 <= f + i - 1 < FR:
                h = h + jnp.dot(
                    act[f + i - 1], w_ref[3 * C * i : 3 * C * (i + 1)], preferred_element_type=jnp.float32
                )
        if last:
            low = h.astype(jnp.bfloat16)
            out_ref[f] = low
            h = low.astype(jnp.float32)
        else:
            out_ref[f] = h
        counted = h * mine
        total = total + jnp.sum(counted.reshape(ROWS // 8, 8, C), axis=0)
        square = square + jnp.sum((counted * h).reshape(ROWS // 8, 8, C), axis=0)
    sums = jnp.concatenate([jnp.sum(total, axis=0, keepdims=True), jnp.sum(square, axis=0, keepdims=True)], axis=0)
    for n in range(NY * NC):
        sums_ref[n] = sums


def layer(index, base, first, last, core, h, part, par, valid, own, weights):
    vmem = pl.BlockSpec(memory_space=pltpu.VMEM)
    hbm = pl.BlockSpec(memory_space=pltpu.HBM)
    out_shape = [
        jax.ShapeDtypeStruct((FR, ROWS, C), jnp.bfloat16 if last else jnp.float32),
        jax.ShapeDtypeStruct((NY * NC, 2, C), jnp.float32),
    ]
    return pl.pallas_call(
        functools.partial(layer_kernel, index, min(index, weights[0].shape[0] - 1), base, first, last, len(weights) - 1),
        out_shape=tuple(out_shape),
        in_specs=[pl.BlockSpec(memory_space=pltpu.SMEM)] + [vmem] * 5 + [hbm] * len(weights),
        out_specs=(vmem, vmem),
        scratch_shapes=[
            pltpu.VMEM((FR, ROWS, 3 * C), jnp.bfloat16),
            pltpu.VMEM((K, C), jnp.bfloat16),
            pltpu.SemaphoreType.DMA((2,)),
        ],
        compiler_params=pltpu.CompilerParams(vmem_limit_bytes=16 * 1024 * 1024),
        cost_estimate=pl.CostEstimate(flops=1200000000, bytes_accessed=4000000, transcendentals=300000),
        name="layer",
    )(core, h, part, par, valid, own, *weights)


def ordered_kernel(plane, half, *refs):
    sources, (keep_ref, send_ref, x_ref, wide, line, sem) = refs[:NZ], refs[NZ:]
    for z in range(NZ):

        @pl.when(plane[0] == z)
        def _():
            copy = pltpu.make_async_copy(sources[z], x_ref, sem)
            copy.start()
            copy.wait()

    core = half[0]
    for f in range(FR):
        for lane in range(0, C, 128):
            wide[...] = x_ref[f, :, lane : lane + 128].astype(jnp.float32)
            for a in range(STRIPS):
                line[a * SPAN : (a + 1) * SPAN] = wide[pl.ds(a, SPAN, stride=STRIPS)]
            for k in range(2):
                lo = pl.multiple_of(HALO + 128 * k + 64 * core, 16)
                keep_ref[k, f, :, lane : lane + 128] = line[pl.ds(lo, 64)].astype(jnp.bfloat16)
                lo = pl.multiple_of(HALO + 128 * k + 64 * (1 - core), 16)
                send_ref[k, f, :, lane : lane + 128] = line[pl.ds(lo, 64)].astype(jnp.bfloat16)


def ordered(plane, core, sources):
    vmem = pl.BlockSpec(memory_space=pltpu.VMEM)
    half = jax.ShapeDtypeStruct((2, FR, 64, C), jnp.bfloat16)
    return pl.pallas_call(
        ordered_kernel,
        out_shape=(half, half),
        in_specs=[pl.BlockSpec(memory_space=pltpu.SMEM)] * 2 + [pl.BlockSpec(memory_space=pl.ANY)] * NZ,
        out_specs=(vmem, vmem),
        scratch_shapes=[
            pltpu.VMEM((FR, ROWS, C), jnp.bfloat16),
            pltpu.VMEM((ROWS, 128), jnp.float32),
            pltpu.VMEM((ROWS, 128), jnp.float32),
            pltpu.SemaphoreType.DMA,
        ],
        compiler_params=pltpu.CompilerParams(vmem_limit_bytes=8 * 1024 * 1024),
        cost_estimate=pl.CostEstimate(flops=2000000, bytes_accessed=2000000, transcendentals=0),
        name="ordered",
    )(plane, core, *sources)


def halves_kernel(plane, half, w_hbm, two_hbm, one_hbm, last_hbm, held, sem):
    size = K // 2
    z, core = plane[0], half[0]
    rows = pl.ds(pl.multiple_of(core * size, size), size)

    def carry(*targets):
        takes = [pltpu.make_async_copy(w_hbm.at[i, rows], held.at[i], sem.at[i]) for i in range(len(targets))]
        gives = [pltpu.make_async_copy(held.at[i], target, sem.at[2 + i]) for i, target in enumerate(targets)]
        for take in takes:
            take.start()
        for take, give in zip(takes, gives):
            take.wait()
            give.start()
        for give in gives:
            give.wait()

    @pl.when(z == 2)
    def _():
        carry(two_hbm.at[0], two_hbm.at[1])

    @pl.when(z == 3)
    def _():
        carry(one_hbm.at[0], last_hbm.at[0])

    @pl.when((z == 4) | (z == 5) | (z == 6))
    def _():
        carry(one_hbm.at[0])


def halves(plane, core, weight):
    hbm = pl.BlockSpec(memory_space=pltpu.HBM)
    return pl.pallas_call(
        halves_kernel,
        out_shape=tuple(jax.ShapeDtypeStruct((n, K // 2, C), jnp.bfloat16) for n in (2, 1, 1)),
        in_specs=[pl.BlockSpec(memory_space=pltpu.SMEM)] * 2 + [hbm],
        out_specs=(hbm, hbm, hbm),
        scratch_shapes=[pltpu.VMEM((2, K // 2, C), jnp.bfloat16), pltpu.SemaphoreType.DMA((4,))],
        compiler_params=pltpu.CompilerParams(vmem_limit_bytes=60 * 1024 * 1024),
        cost_estimate=pl.CostEstimate(flops=1000000, bytes_accessed=5000000, transcendentals=0),
        name="halves",
    )(plane, core, weight)


def moved(value, moves, axis="z"):
    return lax.ppermute(value, axis, moves)


def swapped(value):
    return moved(value, [(0, 1), (1, 0)], "c")


def program(clean, noise, timestep, lift, norm_gain, norm_bias, conv_weight, time_proj):
    z, y, c = (lax.axis_index(a) for a in ("z", "y", "c"))
    place = 2 * y + c
    core = c.reshape(1).astype(jnp.int32)
    own_w = conv_weight[0].reshape(2, K, C)
    plane = z.reshape(1).astype(jnp.int32)
    half, one, other = halves(plane, core, own_w)
    near = moved(half, [(2, 1)])

    steps_f = timestep.astype(jnp.float32)
    level = jnp.cos(math.pi / 2.0 * (steps_f / STEPS + 0.008) / 1.008) ** 2
    noisy = jnp.sqrt(level)[:, None, None] * clean + jnp.sqrt(1.0 - level)[:, None, None] * noise
    sent = jnp.broadcast_to(noisy[None, :, None], (NY, NX, NC, FR, 64)).reshape(NY * NX * NC, FR * 64)
    lifts = jnp.stack([lift, lift * lift])
    line = lax.all_to_all(sent, TM, 0, 0, tiled=True)
    part = (jnp.stack([line, line * line]).sum(axis=(1, 2))[:, None] * lifts)[None]
    line = line.reshape(NY * NX * NC, FR, 64).transpose(1, 0, 2).reshape(FR, -1)
    line = jnp.pad(line, ((0, 0), (HALO, HALO)))
    mine = lax.dynamic_slice_in_dim(line, place * OWN, ROWS, axis=1)
    mine = mine.reshape(FR, STRIPS, SPAN).transpose(0, 2, 1).reshape(FR, ROWS)
    h = (mine[..., None] * lift).astype(jnp.bfloat16)

    row = lax.broadcasted_iota(jnp.int32, (ROWS, 128), 0)
    frame = (row % STRIPS) * SPAN + row // STRIPS
    when = frame + place * OWN - HALO
    valid = ((when >= 0) & (when < OWN * NY * NC)).astype(jnp.float32)
    own = ((frame >= HALO) & (frame < HALO + OWN)).astype(jnp.float32)

    few = C // 2
    freqs = jnp.exp(-math.log(10000.0) * jnp.arange(few, dtype=jnp.float32) / few)
    angles = steps_f[:, None] * freqs[None, :]
    emb = jnp.concatenate([jnp.sin(angles), jnp.cos(angles)], axis=1).astype(jnp.bfloat16)
    temb = jnp.dot(emb, time_proj[0], preferred_element_type=jnp.float32)
    temb = lax.dynamic_slice_in_dim(temb, lax.axis_index("x"), 1, axis=0)
    own_p = jnp.concatenate(
        [norm_gain[0, 0:1], norm_bias[0, 0:1], norm_gain[0, 1:2], norm_bias[0, 1:2], temb, jnp.zeros((3, C), jnp.float32)]
    )
    p2 = moved(own_p, [(2, 1), (6, 7), (4, 3)])
    h, part, valid, own, own_p, core = lax.optimization_barrier((h, part, valid, own, own_p, core))

    def run(index, last, h, part, p, weights, base=0):
        return layer(index, base, index == 0, last, core, h, part, p, valid, own, weights)

    def stats(part, *settled):
        part, *settled = lax.optimization_barrier((part, *settled))
        part = lax.all_to_all(part, ROW, 0, 0, tiled=True)
        return (part, *settled) if settled else part

    own_w = (own_w,)
    h, part = run(0, False, h, part, own_p, own_w)
    h, part = run(1, True, h, stats(part), own_p, own_w)
    ret0 = h
    hopped = moved(h, [(0, 1)])
    part, p2 = stats(part, p2)
    part, one, other, sent_p = lax.optimization_barrier((part, one, other, own_p))
    part = moved(part, [(0, 1)])
    p3 = moved(jnp.concatenate([sent_p, p2]), [(3, 1), (5, 7)])
    w35 = moved(one, [(3, 1), (5, 7)])
    w3b = moved(other, [(3, 1)])
    w46 = moved(one, [(4, 1), (6, 7)])
    h, part = lax.optimization_barrier((hopped, part))
    h, part = run(0, False, h, part, own_p, own_w)
    h, part = run(1, True, h, stats(part), own_p, own_w)
    ret1 = h
    near = (near, swapped(near))
    h, part = run(0, False, h, stats(part), p2, near)
    h, part = run(1, True, h, stats(part), p2, near)
    ret2 = moved(h, [(1, 2)])
    w35 = (w35, swapped(w35))
    part, p3 = stats(part, p3)
    h, part = run(0, False, h, part, p3, w35)
    w3b = (w3b, swapped(w3b))
    h, part = run(1, True, h, stats(part), p3, w3b)
    back3 = h
    w46 = (w46, swapped(w46))
    h, part = run(0, True, h, stats(part), p3, w46, 8)
    hopped = moved(h, [(1, 7)])
    part = moved(stats(part), [(1, 7)])
    ret3 = moved(back3, [(1, 3)])
    ret4 = moved(h, [(1, 4)])
    h, part = lax.optimization_barrier((hopped, part))
    h, part = run(0, True, h, part, p3, w35)
    ret5 = moved(h, [(7, 5)])
    h, part = run(0, True, h, stats(part), p2, w46)
    ret6 = moved(h, [(7, 6)])
    h, part = run(0, True, h, stats(part), own_p, own_w)
    ret7 = h

    keep, send = ordered(plane, core, [ret0, ret1, ret2, ret3, ret4, ret5, ret6, ret7])
    got = swapped(send)
    blocks = jnp.where(c == 0, jnp.concatenate([keep, got]), jnp.concatenate([got, keep]))
    return lax.all_to_all(blocks, "x", 0, 0, tiled=True)[None]


def solution(mesh):
    grid = Mesh(mesh.devices.reshape(NZ, NY, NX, NC), ("z", "y", "x", "c"))
    in_specs = (
        P(None, None, TM),
        P(None, None, TM),
        P(),
        P(),
        P("z", None, None),
        P("z", None, None),
        P("z", None, None, None, None, None),
        P("z", None, None),
    )
    return jax.shard_map(program, mesh=grid, in_specs=in_specs, out_specs=P("z", None, None, TM, None), check_vma=False)
```

```python
import functools
import math

import jax
import jax.numpy as jnp
from jax import lax
from jax.experimental import pallas as pl
from jax.experimental.pallas import tpu as pltpu
from jax.sharding import Mesh
from jax.sharding import PartitionSpec as P

C = 256
STEPS = 1000
NZ, NY, NX, NC = 8, 4, 4, 2
FR = 4
OWN = 256
HALO = 16
STRIPS = 16
SPAN = (OWN + 2 * HALO) // STRIPS
ROWS = STRIPS * SPAN
POSITIONS = FR * OWN * NY * NC
COUNT = POSITIONS * 8
K = 9 * C
TM = ("y", "x", "c")
ROW = ("y", "c")


def group_total(x):
    lane = lax.broadcasted_iota(jnp.int32, x.shape, 1)
    for step in (1, 2, 4):
        up = pltpu.roll(x, C - step, 1)
        down = pltpu.roll(x, step, 1)
        x = x + jnp.where((lane & step) == 0, up, down)
    return x


def layer_kernel(level_plane, index, slot, base, first, last, split, plane, core, h_ref, part_ref, par_ref, valid_ref, own_ref, *refs):
    weights, rest = refs[: 1 + split], refs[1 + split :]
    out_ref, sums_ref = rest[:2]
    act, w_ref, sem = rest[2:]
    if split:
        size = K // 2
        lows = (core[0] * size, (1 - core[0]) * size)
        fetches = [
            pltpu.make_async_copy(w.at[slot], w_ref.at[pl.ds(pl.multiple_of(lo, size), size)], sem.at[n])
            for n, (w, lo) in enumerate(zip(weights, lows))
        ]
    else:
        fetches = [pltpu.make_async_copy(weights[0].at[slot], w_ref, sem.at[0])]
    for fetch in fetches:
        fetch.start()
    sums = jnp.sum(part_ref[...], axis=0)
    total, square = sums[0:1], sums[1:2]
    gain, bias, temb = (par_ref[base + r : base + r + 1] for r in (2 * index, 2 * index + 1, 4))
    if first:
        square = square + 2.0 * temb * total + POSITIONS * temb * temb
        total = total + POSITIONS * temb
    both = group_total(jnp.concatenate([total, square, jnp.zeros((6, C), jnp.float32)], axis=0))
    mean = both[0:1] / COUNT
    var = both[1:2] / COUNT - mean * mean
    scale = 0.5 * lax.rsqrt(var + 1e-05) * gain
    shift = 0.5 * bias
    centre = mean - temb if first else mean

    def activate(f, _):
        for lo in range(0, ROWS, 2 * STRIPS):
            hi = lo + 2 * STRIPS
            h = h_ref[f, lo:hi].astype(jnp.float32)
            half = (h - centre) * scale + shift
            valid = valid_ref[lo:hi]
            a = (half + half * jnp.tanh(half)) * jnp.concatenate([valid, valid], axis=1)
            b = a.astype(jnp.bfloat16)
            act[f, lo:hi, C : 2 * C] = b
            if hi < ROWS:
                act[f, lo + STRIPS : hi + STRIPS, 0:C] = b
            else:
                act[f, hi - STRIPS : hi, 0:C] = b[:STRIPS]
                act[f, 0:STRIPS, 0:C] = pltpu.roll(a[STRIPS:], 1, 0).astype(jnp.bfloat16)
            if lo > 0:
                act[f, lo - STRIPS : hi - STRIPS, 2 * C : 3 * C] = b
            else:
                act[f, 0:STRIPS, 2 * C : 3 * C] = b[STRIPS:]
                act[f, ROWS - STRIPS : ROWS, 2 * C : 3 * C] = pltpu.roll(a[:STRIPS], STRIPS - 1, 0).astype(jnp.bfloat16)
        return 0

    lax.fori_loop(0, jnp.where(plane[0] == level_plane, FR, 0), activate, 0)
    for fetch in fetches:
        fetch.wait()
    total = jnp.zeros((8, C), jnp.float32)
    square = jnp.zeros((8, C), jnp.float32)
    mine = jnp.concatenate([own_ref[...], own_ref[...]], axis=1)
    for f in range(FR):
        h = h_ref[f].astype(jnp.float32)
        if first:
            h = h + temb
        for i in range(3):
            if 0 <= f + i - 1 < FR:
                h = h + jnp.dot(
                    act[f + i - 1], w_ref[3 * C * i : 3 * C * (i + 1)], preferred_element_type=jnp.float32
                )
        if last:
            low = h.astype(jnp.bfloat16)
            out_ref[f] = low
            h = low.astype(jnp.float32)
        else:
            out_ref[f] = h
        counted = h * mine
        total = total + jnp.sum(counted.reshape(ROWS // 8, 8, C), axis=0)
        square = square + jnp.sum((counted * h).reshape(ROWS // 8, 8, C), axis=0)
    sums = jnp.concatenate([jnp.sum(total, axis=0, keepdims=True), jnp.sum(square, axis=0, keepdims=True)], axis=0)
    for n in range(NY * NC):
        sums_ref[n] = sums


def layer(level_plane, index, base, first, last, plane, core, h, part, par, valid, own, weights):
    vmem = pl.BlockSpec(memory_space=pltpu.VMEM)
    hbm = pl.BlockSpec(memory_space=pltpu.HBM)
    out_shape = [
        jax.ShapeDtypeStruct((FR, ROWS, C), jnp.bfloat16 if last else jnp.float32),
        jax.ShapeDtypeStruct((NY * NC, 2, C), jnp.float32),
    ]
    return pl.pallas_call(
        functools.partial(layer_kernel, level_plane, index, min(index, weights[0].shape[0] - 1), base, first, last, len(weights) - 1),
        out_shape=tuple(out_shape),
        in_specs=[pl.BlockSpec(memory_space=pltpu.SMEM)] * 2 + [vmem] * 5 + [hbm] * len(weights),
        out_specs=(vmem, vmem),
        scratch_shapes=[
            pltpu.VMEM((FR, ROWS, 3 * C), jnp.bfloat16),
            pltpu.VMEM((K, C), jnp.bfloat16),
            pltpu.SemaphoreType.DMA((2,)),
        ],
        compiler_params=pltpu.CompilerParams(vmem_limit_bytes=16 * 1024 * 1024),
        cost_estimate=pl.CostEstimate(flops=1200000000, bytes_accessed=4000000, transcendentals=300000),
        name="layer",
    )(plane, core, h, part, par, valid, own, *weights)


def ordered_kernel(plane, half, *refs):
    sources, (keep_ref, send_ref, x_ref, wide, line, sem) = refs[:NZ], refs[NZ:]
    for z in range(NZ):

        @pl.when(plane[0] == z)
        def _():
            copy = pltpu.make_async_copy(sources[z], x_ref, sem)
            copy.start()
            copy.wait()

    core = half[0]
    for f in range(FR):
        for lane in range(0, C, 128):
            wide[...] = x_ref[f, :, lane : lane + 128].astype(jnp.float32)
            for a in range(STRIPS):
                line[a * SPAN : (a + 1) * SPAN] = wide[pl.ds(a, SPAN, stride=STRIPS)]
            for k in range(2):
                lo = pl.multiple_of(HALO + 128 * k + 64 * core, 16)
                keep_ref[k, f, :, lane : lane + 128] = line[pl.ds(lo, 64)].astype(jnp.bfloat16)
                lo = pl.multiple_of(HALO + 128 * k + 64 * (1 - core), 16)
                send_ref[k, f, :, lane : lane + 128] = line[pl.ds(lo, 64)].astype(jnp.bfloat16)


def ordered(plane, core, sources):
    vmem = pl.BlockSpec(memory_space=pltpu.VMEM)
    half = jax.ShapeDtypeStruct((2, FR, 64, C), jnp.bfloat16)
    return pl.pallas_call(
        ordered_kernel,
        out_shape=(half, half),
        in_specs=[pl.BlockSpec(memory_space=pltpu.SMEM)] * 2 + [pl.BlockSpec(memory_space=pl.ANY)] * NZ,
        out_specs=(vmem, vmem),
        scratch_shapes=[
            pltpu.VMEM((FR, ROWS, C), jnp.bfloat16),
            pltpu.VMEM((ROWS, 128), jnp.float32),
            pltpu.VMEM((ROWS, 128), jnp.float32),
            pltpu.SemaphoreType.DMA,
        ],
        compiler_params=pltpu.CompilerParams(vmem_limit_bytes=8 * 1024 * 1024),
        cost_estimate=pl.CostEstimate(flops=2000000, bytes_accessed=2000000, transcendentals=0),
        name="ordered",
    )(plane, core, *sources)


def halves_kernel(plane, half, w_hbm, two_hbm, one_hbm, last_hbm, held, sem):
    size = K // 2
    z, core = plane[0], half[0]
    rows = pl.ds(pl.multiple_of(core * size, size), size)

    def carry(*targets):
        takes = [pltpu.make_async_copy(w_hbm.at[i, rows], held.at[i], sem.at[i]) for i in range(len(targets))]
        gives = [pltpu.make_async_copy(held.at[i], target, sem.at[2 + i]) for i, target in enumerate(targets)]
        for take in takes:
            take.start()
        for take, give in zip(takes, gives):
            take.wait()
            give.start()
        for give in gives:
            give.wait()

    @pl.when(z == 2)
    def _():
        carry(two_hbm.at[0], two_hbm.at[1])

    @pl.when(z == 3)
    def _():
        carry(one_hbm.at[0], last_hbm.at[0])

    @pl.when((z == 4) | (z == 5) | (z == 6))
    def _():
        carry(one_hbm.at[0])


def halves(plane, core, weight):
    hbm = pl.BlockSpec(memory_space=pltpu.HBM)
    return pl.pallas_call(
        halves_kernel,
        out_shape=tuple(jax.ShapeDtypeStruct((n, K // 2, C), jnp.bfloat16) for n in (2, 1, 1)),
        in_specs=[pl.BlockSpec(memory_space=pltpu.SMEM)] * 2 + [hbm],
        out_specs=(hbm, hbm, hbm),
        scratch_shapes=[pltpu.VMEM((2, K // 2, C), jnp.bfloat16), pltpu.SemaphoreType.DMA((4,))],
        compiler_params=pltpu.CompilerParams(vmem_limit_bytes=60 * 1024 * 1024),
        cost_estimate=pl.CostEstimate(flops=1000000, bytes_accessed=5000000, transcendentals=0),
        name="halves",
    )(plane, core, weight)


def moved(value, moves, axis="z"):
    return lax.ppermute(value, axis, moves)


def swapped(value):
    return moved(value, [(0, 1), (1, 0)], "c")


def program(clean, noise, timestep, lift, norm_gain, norm_bias, conv_weight, time_proj):
    z, y, c = (lax.axis_index(a) for a in ("z", "y", "c"))
    place = 2 * y + c
    core = c.reshape(1).astype(jnp.int32)
    own_w = conv_weight[0].reshape(2, K, C)
    plane = z.reshape(1).astype(jnp.int32)
    half, one, other = halves(plane, core, own_w)
    near = moved(half, [(2, 1)])

    steps_f = timestep.astype(jnp.float32)
    level = jnp.cos(math.pi / 2.0 * (steps_f / STEPS + 0.008) / 1.008) ** 2
    noisy = jnp.sqrt(level)[:, None, None] * clean + jnp.sqrt(1.0 - level)[:, None, None] * noise
    sent = jnp.broadcast_to(noisy[None, :, None], (NY, NX, NC, FR, 64)).reshape(NY * NX * NC, FR * 64)
    lifts = jnp.stack([lift, lift * lift])
    line = lax.all_to_all(sent, TM, 0, 0, tiled=True)
    part = (jnp.stack([line, line * line]).sum(axis=(1, 2))[:, None] * lifts)[None]
    line = line.reshape(NY * NX * NC, FR, 64).transpose(1, 0, 2).reshape(FR, -1)
    line = jnp.pad(line, ((0, 0), (HALO, HALO)))
    mine = lax.dynamic_slice_in_dim(line, place * OWN, ROWS, axis=1)
    mine = mine.reshape(FR, STRIPS, SPAN).transpose(0, 2, 1).reshape(FR, ROWS)
    h = (mine[..., None] * lift).astype(jnp.bfloat16)

    row = lax.broadcasted_iota(jnp.int32, (ROWS, 128), 0)
    frame = (row % STRIPS) * SPAN + row // STRIPS
    when = frame + place * OWN - HALO
    valid = ((when >= 0) & (when < OWN * NY * NC)).astype(jnp.float32)
    own = ((frame >= HALO) & (frame < HALO + OWN)).astype(jnp.float32)

    few = C // 2
    freqs = jnp.exp(-math.log(10000.0) * jnp.arange(few, dtype=jnp.float32) / few)
    angles = steps_f[:, None] * freqs[None, :]
    emb = jnp.concatenate([jnp.sin(angles), jnp.cos(angles)], axis=1).astype(jnp.bfloat16)
    temb = jnp.dot(emb, time_proj[0], preferred_element_type=jnp.float32)
    temb = lax.dynamic_slice_in_dim(temb, lax.axis_index("x"), 1, axis=0)
    own_p = jnp.concatenate(
        [norm_gain[0, 0:1], norm_bias[0, 0:1], norm_gain[0, 1:2], norm_bias[0, 1:2], temb, jnp.zeros((3, C), jnp.float32)]
    )
    p2 = moved(own_p, [(2, 1), (6, 7), (4, 3)])
    h, part, valid, own, own_p, core = lax.optimization_barrier((h, part, valid, own, own_p, core))

    def run(n, index, last, h, part, p, weights, base=0):
        return layer(0 if n < 2 else 1 if n < 9 else 7, index, base, index == 0, last, plane, core, h, part, p, valid, own, weights)

    def stats(part, *settled):
        part, *settled = lax.optimization_barrier((part, *settled))
        part = lax.all_to_all(part, ROW, 0, 0, tiled=True)
        return (part, *settled) if settled else part

    own_w = (own_w,)
    h, part = run(0, 0, False, h, part, own_p, own_w)
    h, part = run(1, 1, True, h, stats(part), own_p, own_w)
    ret0 = h
    hopped = moved(h, [(0, 1)])
    part, p2 = stats(part, p2)
    part, one, other, sent_p = lax.optimization_barrier((part, one, other, own_p))
    part = moved(part, [(0, 1)])
    p3 = moved(jnp.concatenate([sent_p, p2]), [(3, 1), (5, 7)])
    w35 = moved(one, [(3, 1), (5, 7)])
    w3b = moved(other, [(3, 1)])
    w46 = moved(one, [(4, 1), (6, 7)])
    h, part = lax.optimization_barrier((hopped, part))
    h, part = run(2, 0, False, h, part, own_p, own_w)
    h, part = run(3, 1, True, h, stats(part), own_p, own_w)
    ret1 = h
    near = (near, swapped(near))
    h, part = run(4, 0, False, h, stats(part), p2, near)
    h, part = run(5, 1, True, h, stats(part), p2, near)
    ret2 = moved(h, [(1, 2)])
    w35 = (w35, swapped(w35))
    part, p3 = stats(part, p3)
    h, part = run(6, 0, False, h, part, p3, w35)
    w3b = (w3b, swapped(w3b))
    h, part = run(7, 1, True, h, stats(part), p3, w3b)
    back3 = h
    w46 = (w46, swapped(w46))
    h, part = run(8, 0, True, h, stats(part), p3, w46, 8)
    hopped = moved(h, [(1, 7)])
    part = moved(stats(part), [(1, 7)])
    ret3 = moved(back3, [(1, 3)])
    ret4 = moved(h, [(1, 4)])
    h, part = lax.optimization_barrier((hopped, part))
    h, part = run(9, 0, True, h, part, p3, w35)
    ret5 = moved(h, [(7, 5)])
    h, part = run(10, 0, True, h, stats(part), p2, w46)
    ret6 = moved(h, [(7, 6)])
    h, part = run(11, 0, True, h, stats(part), own_p, own_w)
    ret7 = h

    keep, send = ordered(plane, core, [ret0, ret1, ret2, ret3, ret4, ret5, ret6, ret7])
    got = swapped(send)
    blocks = jnp.where(c == 0, jnp.concatenate([keep, got]), jnp.concatenate([got, keep]))
    return lax.all_to_all(blocks, "x", 0, 0, tiled=True)[None]


def solution(mesh):
    grid = Mesh(mesh.devices.reshape(NZ, NY, NX, NC), ("z", "y", "x", "c"))
    in_specs = (
        P(None, None, TM),
        P(None, None, TM),
        P(),
        P(),
        P("z", None, None),
        P("z", None, None),
        P("z", None, None, None, None, None),
        P("z", None, None),
    )
    return jax.shard_map(program, mesh=grid, in_specs=in_specs, out_specs=P("z", None, None, TM, None), check_vma=False)
```
